8 devices in a mesh: dp: 1 (over z), tp: 8 (over x, y, core).
Axes of the slice: x: 2, y: 2, z: 1, core: 2. Of those that a mesh axis runs over, the one named last changes fastest.
Arguments:
- x: bfloat16 [2048, 2048], P('dp')
- dy: bfloat16 [2048, 2048], P('dp')
- gate: bfloat16 [2048, 5120], P('dp', 'tp')
- up: bfloat16 [2048, 5120], P('dp', 'tp')
- w_gate: bfloat16 [2048, 5120], P(None, 'tp')
- w_up: bfloat16 [2048, 5120], P(None, 'tp')
- w_down: bfloat16 [5120, 2048], P('tp')
Outputs:
- output 1: bfloat16 [2048, 2048], P('dp')
- output 2: bfloat16 [2048, 5120], P('dp', 'tp')
- output 3: bfloat16 [2048, 5120], P('dp', 'tp')
- output 4: bfloat16 [5120, 2048], P(('dp', 'tp'))
All inputs are finite; a program needn't handle non-finite values.
Results may differ from the reference program's by a relative error of at most 0.012.
Values are sent between devices in bfloat16 or wider.
A program may use at most 2 GiB of HBM per device.

```python
import jax
import jax.numpy as jnp

ROWS = 2048
D = 2048
FF = 5120


def act(gate, up):
    return jax.nn.gelu(gate) * up


def setup_inputs(seed: int = 0, part: int = 0) -> dict:
    kx, ky, ka, kb, kg, ku, kd = jax.random.split(jax.random.key(seed), 7)
    kx, ky, ka, kb = (jax.random.fold_in(k, part) for k in (kx, ky, ka, kb))
    drawn = {
        "x": jax.random.normal(kx, (ROWS, D), jnp.float32),
        "dy": jax.random.normal(ky, (ROWS, D), jnp.float32),
        "gate": jax.random.normal(ka, (ROWS, FF), jnp.float32),
        "up": jax.random.normal(kb, (ROWS, FF), jnp.float32),
        "w_gate": jax.random.normal(kg, (D, FF), jnp.float32) * D**-0.5,
        "w_up": jax.random.normal(ku, (D, FF), jnp.float32) * D**-0.5,
        "w_down": jax.random.normal(kd, (FF, D), jnp.float32) * FF**-0.5,
    }
    return {k: v.astype(jnp.bfloat16) for k, v in drawn.items()}


def reference(x, dy, gate, up, w_gate, w_up, w_down):
    hidden, back = jax.vjp(act, gate.astype(jnp.float32), up.astype(jnp.float32))
    d_hidden = jnp.dot(dy, w_down.T, preferred_element_type=jnp.float32)
    d_gate, d_up = (g.astype(jnp.bfloat16) for g in back(d_hidden))
    dx = jnp.dot(d_gate, w_gate.T, preferred_element_type=jnp.float32) + jnp.dot(d_up, w_up.T, preferred_element_type=jnp.float32)
    dw_gate = jnp.dot(x.T, d_gate, preferred_element_type=jnp.float32)
    dw_up = jnp.dot(x.T, d_up, preferred_element_type=jnp.float32)
    dw_down = jnp.dot(hidden.astype(jnp.bfloat16).T, dy, preferred_element_type=jnp.float32)
    return tuple(g.astype(jnp.bfloat16) for g in (dx, dw_gate, dw_up, dw_down))
```

```python
import functools

import jax
import jax.numpy as jnp
from jax import lax
from jax.experimental import pallas as pl
from jax.experimental.pallas import tpu as pltpu
from jax.sharding import PartitionSpec as P

MESH = pl.DeviceIdType.MESH
BF = jnp.bfloat16
F32 = jnp.float32
T = 256
NC = 8
D = 2048
F = 640
B = 128
L2, L3, L4, L5 = 1, 4, 7, 11
C0 = 0.7978845608028654
C1 = 0.044715


def dot(a, b, dims=((1,), (0,))):
    return lax.dot_general(a, b, (dims, ((), ())), preferred_element_type=F32)


def kernel(
    x_hbm, dy_hbm, gate_hbm, up_hbm, wg_hbm, wu_hbm, wd_hbm,
    dx, dwg, dwu, dwd,
    wcat, wd, dcat, hid, dyc, gc, uc, xp, yp, dh, keep, outs,
    c1s, c1r, p1s, p1r, p2s, p2r,
    in_sem, w_sem, pan_sem,
    c1ss, c1rs, p1ss, p1rs, p2ss, p2rs, gss, grs, cfs, cfr,
):
    me = lax.axis_index("tp")
    c = lax.rem(me, 2)
    y = lax.rem(me // 2, 2)
    x = me // 4
    nx, ny, nc = me + 4 - 8 * x, me + 2 - 4 * y, me + 1 - 2 * c

    def rcopy(src, dst, ss, rs, to):
        return pltpu.make_async_remote_copy(
            src_ref=src, dst_ref=dst, send_sem=ss, recv_sem=rs, device_id={"tp": to}, device_id_type=MESH
        )

    def chunk_loads(k):
        s = lax.rem(k, 2)
        rows = pl.ds(pl.multiple_of(k * T, T), T)
        return [
            pltpu.make_async_copy(dy_hbm.at[rows], dyc.at[s], in_sem.at[0, s]),
            pltpu.make_async_copy(gate_hbm.at[rows], gc.at[s], in_sem.at[1, s]),
            pltpu.make_async_copy(up_hbm.at[rows], uc.at[s], in_sem.at[2, s]),
        ]

    def panel_loads(m):
        s = lax.rem(m, 2)
        cols = pl.ds(pl.multiple_of(m * T, T), T)
        return [
            pltpu.make_async_copy(x_hbm.at[:, cols], xp.at[s], pan_sem.at[0, s]),
            pltpu.make_async_copy(dy_hbm.at[:, cols], yp.at[s], pan_sem.at[1, s]),
        ]

    w_loads = []
    for g in range(4):
        own, kept = g % 2, g // 2
        h = c if own else 1 - c
        for ab in range(2):
            first, second = (x, y) if ab == 0 else (y, x)
            i = first if kept else 1 - first
            for jo in range(2):
                j = second if jo else 1 - second
                src = pl.ds(pl.multiple_of(h * 1024 + ab * 512 + i * 256 + j * 128, B), B)
                dst = pl.ds((g * 4 + ab * 2 + jo) * B, B)
                w_loads.append(pltpu.make_async_copy(wg_hbm.at[src], wcat.at[dst, 0:F], w_sem.at[1 + len(w_loads)]))
                w_loads.append(pltpu.make_async_copy(wu_hbm.at[src], wcat.at[dst, F : 2 * F], w_sem.at[1 + len(w_loads)]))
    wd_load = pltpu.make_async_copy(wd_hbm, wd, w_sem.at[0])

    for cp in chunk_loads(0):
        cp.start()
    wd_load.start()
    for cp in w_loads:
        cp.start()

    barrier = pltpu.get_barrier_semaphore()
    for to in (nx, ny, nc):
        pl.semaphore_signal(barrier, inc=1, device_id={"tp": to}, device_id_type=MESH)
    pl.semaphore_wait(barrier, 3)

    def piece(ref, k, ab, cx, cy, h):
        col = h * 1024 + (cx * 256 + cy * 128 if ab == 0 else 512 + cy * 256 + cx * 128)
        return ref.at[pl.ds(pl.multiple_of(k * T, T), T), pl.ds(pl.multiple_of(col, B), B)]

    def c1_copy(k, part):
        return rcopy(c1s.at[k, part], c1r.at[k, part], c1ss.at[k, part], c1rs.at[k, part], nc)

    def p1_copy(k, ab):
        return rcopy(p1s.at[k, ab], p1r.at[k, ab], p1ss.at[k, ab], p1rs.at[k, ab], ny if ab else nx)

    def p2_copy(k, ab):
        return rcopy(p2s.at[k, ab], p2r.at[k, ab], p2ss.at[k, ab], p2rs.at[k, ab], nx if ab else ny)

    def g_copy(k, ab, kind):
        far, near = (ny, nx) if ab else (nx, ny)
        if kind == 2:
            ref = piece(dx, k, ab, x, 1 - y, c) if ab == 0 else piece(dx, k, ab, 1 - x, y, c)
        else:
            ref = piece(dx, k, ab, x, y, c)
        return rcopy(ref, ref, gss.at[k, ab, kind], grs.at[k, ab, kind], near if kind == 0 else far)

    def cf_copy(k, ab, which):
        cx, cy = ((x, y), (x, 1 - y), (1 - x, y), (1 - x, 1 - y))[which]
        ref = piece(dx, k, ab, cx, cy, c)
        return rcopy(ref, ref, cfs.at[k, ab, which], cfr.at[k, ab, which], nc)

    def s1(k):
        c1_copy(k, 0).wait_recv()
        for ab in range(2):
            rows = pl.ds(ab * 256, 256)
            p1s[k, ab] = (outs[rows] + c1r[k, 0, rows].astype(F32)).astype(BF)
            p1_copy(k, ab).start()

    def s1b(k):
        c1_copy(k, 1).wait_recv()
        keep[k] = keep[k] + c1r[k, 1].astype(F32)

    def s2(k):
        for ab in range(2):
            p1_copy(k, ab).wait_recv()
            rows = pl.ds(ab * 256, B)
            p2s[k, ab] = (keep[k, rows] + p1r[k, ab, 0:B].astype(F32)).astype(BF)
            p2_copy(k, ab).start()
            rows = pl.ds(ab * 256 + B, B)
            keep[k, rows] = keep[k, rows] + p1r[k, ab, B : 2 * B].astype(F32)

    def s3(k):
        for ab in range(2):
            p2_copy(k, ab).wait_recv()
            done = (keep[k, pl.ds(ab * 256 + B, B)] + p2r[k, ab].astype(F32)).astype(BF)
            piece(dx, k, ab, x, y, c)[...] = done.T
            g_copy(k, ab, 0).start()
            g_copy(k, ab, 1).start()
            cf_copy(k, ab, 0).start()

    def s4(k):
        for ab in range(2):
            g_copy(k, ab, 0).wait_recv()
            g_copy(k, ab, 2).start()
            cf_copy(k, ab, 1 if ab == 0 else 2).start()
            g_copy(k, ab, 1).wait_recv()
            cf_copy(k, ab, 2 if ab == 0 else 1).start()

    def s5(k):
        for ab in range(2):
            g_copy(k, ab, 2).wait_recv()
            cf_copy(k, ab, 3).start()

    def exchange(k, lag, fn):
        @pl.when(jnp.logical_and(k >= lag, k < NC + lag))
        def _():
            fn(k - lag)

    def term(k, g, ref):
        cols = pl.ds(pl.multiple_of(k * T, T), T)
        ref[...] = dot(wcat[g * 512 : (g + 1) * 512], dcat[:, cols]).astype(ref.dtype)

    def phase1(k, _):
        slot = lax.rem(k, 2)
        cols = pl.ds(pl.multiple_of(k * T, T), T)
        for cp in chunk_loads(k):
            cp.wait()

        @pl.when(k < NC - 1)
        def _():
            for cp in chunk_loads(k + 1):
                cp.start()

        @pl.when(k == 0)
        def _():
            wd_load.wait()

        @pl.when(jnp.logical_and(k >= 2, k < 4))
        def _():
            for cp in panel_loads(k - 2):
                cp.start()

        dh[...] = dot(wd[...], dyc[slot], ((1,), (1,)))
        for r in range(5):
            rows = slice(r * B, (r + 1) * B)
            g = gc[slot, :, rows].T.astype(F32)
            u = uc[slot, :, rows].T.astype(F32)
            d = dh[rows]
            g2 = g * g
            t = jnp.tanh(g * (C0 + (C0 * C1) * g2))
            cdf = 0.5 + 0.5 * t
            act = g * cdf
            slope = cdf + (act * (1.0 - t)) * (C0 + (3.0 * C0 * C1) * g2)
            hid[rows, cols] = (act * u).astype(BF)
            dcat[rows, cols] = (d * u * slope).astype(BF)
            dcat[F + r * B : F + (r + 1) * B, cols] = (d * act).astype(BF)

        for g in range(4):

            @pl.when(k == 0)
            def _():
                for cp in w_loads[g * 8 : (g + 1) * 8]:
                    cp.wait()

            if g == 0:
                term(k, 0, c1s.at[k, 0])
                c1_copy(k, 0).start()
            elif g == 1:
                term(k, 1, outs)
            elif g == 2:
                term(k, 2, c1s.at[k, 1])
                c1_copy(k, 1).start()
                s1(k)
            else:
                term(k, 3, keep.at[k])
                s1b(k)
        exchange(k, L2, s2)
        exchange(k, L3, s3)
        exchange(k, L4, s4)
        exchange(k, L5, s5)
        return 0

    lax.fori_loop(0, NC, phase1, 0)

    def phase2(m, _):
        slot = lax.rem(m, 2)
        k = NC + m
        at = pl.ds(pl.multiple_of(m * T, T), T)
        for cp in panel_loads(m):
            cp.wait()
        dwg[at] = dot(dcat[0:F], xp[slot]).astype(BF).T
        exchange(k, L2, s2)
        exchange(k, L3, s3)
        dwu[at] = dot(dcat[F : 2 * F], xp[slot]).astype(BF).T
        exchange(k, L4, s4)
        dwd[:, at] = dot(hid[...], yp[slot]).astype(BF)

        @pl.when(m < NC - 2)
        def _():
            for cp in panel_loads(m + 2):
                cp.start()

        exchange(k, L5, s5)
        return 0

    lax.fori_loop(0, NC, phase2, 0)

    def phase3(k, _):
        exchange(k, L4, s4)
        exchange(k, L5, s5)
        return 0

    lax.fori_loop(2 * NC, NC + L5, phase3, 0)

    def finish(k, _):
        for i in range(2):
            c1_copy(k, i).wait_send()
            p1_copy(k, i).wait_send()
            p2_copy(k, i).wait_send()
            for kind in range(3):
                g_copy(k, i, kind).wait_send()
            for which in range(4):
                cf_copy(k, i, which).wait()
        return 0

    lax.fori_loop(0, NC, finish, 0)


def write_out(dx, dwg, dwu, dwd, dx_o, dwg_o, dwu_o, dwd_o, sem):
    copies = []
    for src, dst, parts in ((dx, dx_o, 8), (dwg, dwg_o, 4), (dwu, dwu_o, 4), (dwd, dwd_o, 4)):
        n = src.shape[0] // parts
        for i in range(parts):
            rows = pl.ds(i * n, n)
            copies.append(pltpu.make_async_copy(src.at[rows], dst.at[rows], sem.at[len(copies)]))
    for cp in copies:
        cp.start()
    for cp in copies:
        cp.wait()


def solution(mesh):
    def step(x, dy, gate, up, w_gate, w_up, w_down):
        hbm = pl.BlockSpec(memory_space=pltpu.HBM)
        vmem = pl.BlockSpec(memory_space=pltpu.VMEM)
        shapes = ((D, D), (D, F), (D, F), (F, D))
        dma = pltpu.SemaphoreType.DMA
        args = [pltpu.with_memory_space_constraint(a, pltpu.HBM) for a in (x, dy, gate, up, w_gate, w_up, w_down)]
        results = pl.pallas_call(
            kernel,
            out_shape=tuple(pltpu.VMEM(s, BF) for s in shapes),
            in_specs=[hbm] * 7,
            out_specs=(vmem,) * 4,
            scratch_shapes=[
                pltpu.VMEM((D, 2 * F), BF),
                pltpu.VMEM((F, D), BF),
                pltpu.VMEM((2 * F, D), BF),
                pltpu.VMEM((F, D), BF),
                pltpu.VMEM((2, T, D), BF),
                pltpu.VMEM((2, T, F), BF),
                pltpu.VMEM((2, T, F), BF),
                pltpu.VMEM((2, D, T), BF),
                pltpu.VMEM((2, D, T), BF),
                pltpu.VMEM((F, T), F32),
                pltpu.VMEM((NC, 512, T), F32),
                pltpu.VMEM((512, T), F32),
                pltpu.VMEM((NC, 2, 512, T), BF),
                pltpu.VMEM((NC, 2, 512, T), BF),
                pltpu.VMEM((NC, 2, 256, T), BF),
                pltpu.VMEM((NC, 2, 256, T), BF),
                pltpu.VMEM((NC, 2, 128, T), BF),
                pltpu.VMEM((NC, 2, 128, T), BF),
                dma((3, 2)),
                dma((33,)),
                dma((2, 2)),
                dma((NC, 2)),
                dma((NC, 2)),
                dma((NC, 2)),
                dma((NC, 2)),
                dma((NC, 2)),
                dma((NC, 2)),
                dma((NC, 2, 3)),
                dma((NC, 2, 3)),
                dma((NC, 2, 4)),
                dma((NC, 2, 4)),
            ],
            compiler_params=pltpu.CompilerParams(
                collective_id=0, has_side_effects=True, vmem_limit_bytes=48 * 2**20
            ),
        )(*args)
        return pl.pallas_call(
            write_out,
            out_shape=tuple(jax.ShapeDtypeStruct(s, BF) for s in shapes),
            in_specs=[vmem] * 4,
            out_specs=(hbm,) * 4,
            scratch_shapes=[dma((20,))],
            compiler_params=pltpu.CompilerParams(vmem_limit_bytes=2**20),
        )(*results)

    tokens, columns, rows = P("dp", None), P(None, "tp"), P("tp", None)
    return jax.shard_map(
        step,
        mesh=mesh,
        in_specs=(tokens, tokens, P("dp", "tp"), P("dp", "tp"), columns, columns, rows),
        out_specs=(tokens, P("dp", "tp"), P("dp", "tp"), P(("dp", "tp"), None)),
        check_vma=False,
    )
```

```python
import functools

import jax
import jax.numpy as jnp
from jax import lax
from jax.experimental import pallas as pl
from jax.experimental.pallas import tpu as pltpu
from jax.sharding import PartitionSpec as P

MESH = pl.DeviceIdType.MESH
BF = jnp.bfloat16
F32 = jnp.float32
T = 256
NC = 8
D = 2048
F = 640
B = 128
L2, L3, L4, L5 = 1, 4, 7, 11
C0 = 0.7978845608028654
C1 = 0.044715


def dot(a, b, dims=((1,), (0,))):
    return lax.dot_general(a, b, (dims, ((), ())), preferred_element_type=F32)


def kernel(
    x_hbm, dy_hbm, gate_hbm, up_hbm, wg_hbm, wu_hbm, wd_hbm,
    dx, dwg, dwu, dwd,
    wcat, wd, dcat, hid, dyc, guc, pan, dh, keep, outs,
    c1s, c1r, p1s, p1r, p2s, p2r,
    dy_sem, gu_sem, wd_sem, w_sem, pan_sem,
    c1_sem, p1_sem, p2_sem, g01_sem, g2_sem, cf_sem, sent,
):
    me = lax.axis_index("tp")
    c = lax.rem(me, 2)
    y = lax.rem(me // 2, 2)
    x = me // 4
    nx, ny, nc = me + 4 - 8 * x, me + 2 - 4 * y, me + 1 - 2 * c

    barrier = pltpu.get_barrier_semaphore()
    for to in (nx, ny, nc):
        pl.semaphore_signal(barrier, inc=1, device_id={"tp": to}, device_id_type=MESH)

    def rcopy(src, dst, ss, rs, to):
        return pltpu.make_async_remote_copy(
            src_ref=src, dst_ref=dst, send_sem=ss, recv_sem=rs, device_id={"tp": to}, device_id_type=MESH
        )

    def take(ref, sem):
        pltpu.make_async_copy(ref, ref, sem).wait()

    def load_gu(k, s):
        rows = pl.ds(pl.multiple_of(k * T, T), T)
        pltpu.make_async_copy(gate_hbm.at[rows], guc.at[s, 0], gu_sem.at[s]).start()
        pltpu.make_async_copy(up_hbm.at[rows], guc.at[s, 1], gu_sem.at[s]).start()

    def load_chunk(k, s):
        rows = pl.ds(pl.multiple_of(k * T, T), T)
        pltpu.make_async_copy(dy_hbm.at[rows], dyc.at[s], dy_sem.at[s]).start()
        load_gu(k, s)

    def load_panel(m, s):
        cols = pl.ds(pl.multiple_of(m * T, T), T)
        pltpu.make_async_copy(x_hbm.at[:, cols], pan.at[s, 0], pan_sem.at[s]).start()
        pltpu.make_async_copy(dy_hbm.at[:, cols], pan.at[s, 1], pan_sem.at[s]).start()

    def load_w(g):
        own, kept = g % 2, g // 2
        h = c if own else 1 - c
        for ab in range(2):
            first, second = (x, y) if ab == 0 else (y, x)
            i = first if kept else 1 - first
            for jo in range(2):
                j = second if jo else 1 - second
                src = pl.ds(pl.multiple_of(h * 1024 + ab * 512 + i * 256 + j * 128, B), B)
                dst = pl.ds((g * 4 + ab * 2 + jo) * B, B)
                pltpu.make_async_copy(wg_hbm.at[src], wcat.at[dst, 0:F], w_sem.at[g]).start()
                pltpu.make_async_copy(wu_hbm.at[src], wcat.at[dst, F : 2 * F], w_sem.at[g]).start()

    def piece(ref, k, ab, cx, cy, h):
        col = h * 1024 + (cx * 256 + cy * 128 if ab == 0 else 512 + cy * 256 + cx * 128)
        return ref.at[pl.ds(pl.multiple_of(k * T, T), T), pl.ds(pl.multiple_of(col, B), B)]

    def c1_send(k, part):
        rcopy(c1s.at[k, part], c1r.at[k, part], sent.at[0], c1_sem.at[k, part], nc).start()

    def g_send(k, ab, kind):
        far, near = (ny, nx) if ab else (nx, ny)
        if kind == 2:
            ref = piece(dx, k, ab, x, 1 - y, c) if ab == 0 else piece(dx, k, ab, 1 - x, y, c)
        else:
            ref = piece(dx, k, ab, x, y, c)
        rcopy(ref, ref, sent.at[3], (g2_sem if kind == 2 else g01_sem).at[k], near if kind == 0 else far).start()

    def cf_send(k, ab, which):
        cx, cy = ((x, y), (x, 1 - y), (1 - x, y), (1 - x, 1 - y))[which]
        ref = piece(dx, k, ab, cx, cy, c)
        rcopy(ref, ref, sent.at[4], cf_sem, nc).start()

    @jax.named_scope("s1")
    def s1(k):
        take(c1r.at[k, 0], c1_sem.at[k, 0])
        for ab in range(2):
            rows = pl.ds(ab * 256, 256)
            p1s[k, ab] = (outs[rows] + c1r[k, 0, rows].astype(F32)).astype(BF)
            rcopy(p1s.at[k, ab], p1r.at[k, ab], sent.at[1], p1_sem.at[k], ny if ab else nx).start()

    @jax.named_scope("s1b")
    def s1b(k):
        take(c1r.at[k, 1], c1_sem.at[k, 1])
        keep[k] = keep[k] + c1r[k, 1].astype(F32)

    @jax.named_scope("s2")
    def s2(k):
        take(p1r.at[k], p1_sem.at[k])
        for ab in range(2):
            rows = pl.ds(ab * 256, B)
            p2s[k, ab] = (keep[k, rows] + p1r[k, ab, 0:B].astype(F32)).astype(BF)
            rcopy(p2s.at[k, ab], p2r.at[k, ab], sent.at[2], p2_sem.at[k], nx if ab else ny).start()
        for ab in range(2):
            rows = pl.ds(ab * 256 + B, B)
            keep[k, rows] = keep[k, rows] + p1r[k, ab, B : 2 * B].astype(F32)

    @jax.named_scope("s3")
    def s3(k):
        take(p2r.at[k], p2_sem.at[k])
        for ab in range(2):
            done = (keep[k, pl.ds(ab * 256 + B, B)] + p2r[k, ab].astype(F32)).astype(BF)
            piece(dx, k, ab, x, y, c)[...] = done.T
            g_send(k, ab, 0)
            g_send(k, ab, 1)
            cf_send(k, ab, 0)

    @jax.named_scope("s4")
    def s4(k):
        take(p1r.at[k], g01_sem.at[k])
        for ab in range(2):
            g_send(k, ab, 2)
            cf_send(k, ab, 1)
            cf_send(k, ab, 2)

    @jax.named_scope("s5")
    def s5(k):
        take(p2r.at[k], g2_sem.at[k])
        for ab in range(2):
            cf_send(k, ab, 3)

    def exchange(k, lag, fn):
        @pl.when(jnp.logical_and(k >= lag, k < NC + lag))
        def _():
            fn(k - lag)

    @jax.named_scope("ew")
    def gates(k, slot):
        cols = pl.ds(pl.multiple_of(k * T, T), T)
        for r in range(5):
            rows = slice(r * B, (r + 1) * B)
            g = guc[slot, 0, :, rows].T.astype(F32)
            u = guc[slot, 1, :, rows].T.astype(F32)
            d = dh[rows]
            g2 = g * g
            t = jnp.tanh(g * (C0 + (C0 * C1) * g2))
            cdf = 0.5 + 0.5 * t
            act = g * cdf
            slope = cdf + (act * (1.0 - t)) * (C0 + (3.0 * C0 * C1) * g2)
            hid[rows, cols] = (act * u).astype(BF)
            dcat[rows, cols] = (d * u * slope).astype(BF)
            dcat[F + r * B : F + (r + 1) * B, cols] = (d * act).astype(BF)

    def halves(n):
        return [slice(i * n // 2, (i + 1) * n // 2) for i in range(2)]

    @jax.named_scope("term")
    def term(k, g, ref):
        cols = pl.ds(pl.multiple_of(k * T, T), T)
        for r in halves(512):
            ref[r] = dot(wcat[g * 512 + r.start : g * 512 + r.stop], dcat[:, cols]).astype(ref.dtype)

    for i, d in enumerate(halves(D)):
        pltpu.make_async_copy(wd_hbm.at[:, d], wd.at[:, d], wd_sem.at[i]).start()
        pltpu.make_async_copy(dy_hbm.at[0:T, d], dyc.at[0, :, d], dy_sem.at[i]).start()
    load_gu(0, 0)
    for i, d in enumerate(halves(D)):
        with jax.named_scope("load"):
            take(wd.at[:, d], wd_sem.at[i])
            take(dyc.at[0, :, d], dy_sem.at[i])
        for g in ((0, 1), (2, 3))[i]:
            load_w(g)
        if i:
            load_chunk(1, 1)
        with jax.named_scope("dh"):
            for r in halves(F):
                part = dot(wd[r, d], dyc[0, :, d], ((1,), (1,)))
                dh[r] = dh[r] + part if i else part
    take(guc.at[0], gu_sem.at[0])
    gates(0, 0)
    with jax.named_scope("bar"):
        pl.semaphore_wait(barrier, 3)

    def phase1(k, _):
        for g, ref in enumerate((c1s.at[k, 0], outs, c1s.at[k, 1], keep.at[k])):

            @pl.when(k == 0)
            def _():
                take(wcat.at[g * 512 : (g + 1) * 512], w_sem.at[g])

            term(k, g, ref)
            if g == 0:
                c1_send(k, 0)
            if g == 2:
                c1_send(k, 1)
        s1(k)

        @pl.when(k < NC - 1)
        def _():
            nxt = k + 1
            slot = lax.rem(nxt, 2)
            with jax.named_scope("chunkwait"):
                take(dyc.at[slot], dy_sem.at[slot])
                take(guc.at[slot], gu_sem.at[slot])

            @pl.when(nxt < NC - 1)
            def _():
                load_chunk(nxt + 1, 1 - slot)

            @pl.when(jnp.logical_and(k >= 2, k < 4))
            def _():
                load_panel(k - 2, k - 2)

            with jax.named_scope("dh"):
                for r in halves(F):
                    dh[r] = dot(wd[r], dyc[slot], ((1,), (1,)))
            gates(nxt, slot)

        s1b(k)
        exchange(k, L2, s2)
        exchange(k, L3, s3)
        exchange(k, L4, s4)
        exchange(k, L5, s5)
        return 0

    lax.fori_loop(0, NC, phase1, 0)

    def phase2(m, _):
        slot = lax.rem(m, 2)
        k = NC + m
        at = pl.ds(pl.multiple_of(m * T, T), T)
        take(pan.at[slot], pan_sem.at[slot])
        with jax.named_scope("dwg"):
            for r in halves(F):
                dwg[at, r] = dot(dcat[r], pan[slot, 0]).astype(BF).T
        exchange(k, L2, s2)
        with jax.named_scope("dwu"):
            for r in halves(F):
                dwu[at, r] = dot(dcat[F + r.start : F + r.stop], pan[slot, 0]).astype(BF).T
        exchange(k, L3, s3)
        exchange(k, L4, s4)
        with jax.named_scope("dwd"):
            for r in halves(F):
                dwd[r, at] = dot(hid[r], pan[slot, 1]).astype(BF)

        @pl.when(m < NC - 2)
        def _():
            load_panel(m + 2, slot)

        exchange(k, L5, s5)
        return 0

    lax.fori_loop(0, NC, phase2, 0)

    def phase3(k, _):
        exchange(k, L4, s4)
        exchange(k, L5, s5)
        return 0

    lax.fori_loop(2 * NC, NC + L5, phase3, 0)
    with jax.named_scope("fin"):
        for i, ref in enumerate((c1s, p1s, p2s, dx.at[0:768], dx.at[0:1024])):
            take(ref, sent.at[i])
        take(c1r, cf_sem)


def write_out(dx, dwg, dwu, dwd, dx_o, dwg_o, dwu_o, dwd_o, sem):
    copies = []
    for src, dst, parts in ((dx, dx_o, 8), (dwg, dwg_o, 4), (dwu, dwu_o, 4), (dwd, dwd_o, 4)):
        n = src.shape[0] // parts
        for i in range(parts):
            rows = pl.ds(i * n, n)
            copies.append(pltpu.make_async_copy(src.at[rows], dst.at[rows], sem.at[len(copies)]))
    for cp in copies:
        cp.start()
    for cp in copies:
        cp.wait()


def solution(mesh):
    def step(x, dy, gate, up, w_gate, w_up, w_down):
        hbm = pl.BlockSpec(memory_space=pltpu.HBM)
        vmem = pl.BlockSpec(memory_space=pltpu.VMEM)
        shapes = ((D, D), (D, F), (D, F), (F, D))
        dma = pltpu.SemaphoreType.DMA
        args = [pltpu.with_memory_space_constraint(a, pltpu.HBM) for a in (x, dy, gate, up, w_gate, w_up, w_down)]
        results = pl.pallas_call(
            kernel,
            out_shape=tuple(pltpu.VMEM(s, BF) for s in shapes),
            in_specs=[hbm] * 7,
            out_specs=(vmem,) * 4,
            scratch_shapes=[
                pltpu.VMEM((D, 2 * F), BF),
                pltpu.VMEM((F, D), BF),
                pltpu.VMEM((2 * F, D), BF),
                pltpu.VMEM((F, D), BF),
                pltpu.VMEM((2, T, D), BF),
                pltpu.VMEM((2, 2, T, F), BF),
                pltpu.VMEM((2, 2, D, T), BF),
                pltpu.VMEM((F, T), F32),
                pltpu.VMEM((NC, 512, T), F32),
                pltpu.VMEM((512, T), F32),
                pltpu.VMEM((NC, 2, 512, T), BF),
                pltpu.VMEM((NC, 2, 512, T), BF),
                pltpu.VMEM((NC, 2, 256, T), BF),
                pltpu.VMEM((NC, 2, 256, T), BF),
                pltpu.VMEM((NC, 2, 128, T), BF),
                pltpu.VMEM((NC, 2, 128, T), BF),
                dma((2,)),
                dma((2,)),
                dma((2,)),
                dma((4,)),
                dma((2,)),
                dma((NC, 2)),
                dma((NC,)),
                dma((NC,)),
                dma((NC,)),
                dma((NC,)),
                dma,
                dma((5,)),
            ],
            compiler_params=pltpu.CompilerParams(
                collective_id=0, has_side_effects=True, vmem_limit_bytes=48 * 2**20
            ),
        )(*args)
        return pl.pallas_call(
            write_out,
            out_shape=tuple(jax.ShapeDtypeStruct(s, BF) for s in shapes),
            in_specs=[vmem] * 4,
            out_specs=(hbm,) * 4,
            scratch_shapes=[dma((20,))],
            compiler_params=pltpu.CompilerParams(vmem_limit_bytes=2**20),
        )(*results)

    tokens, columns, rows = P("dp", None), P(None, "tp"), P("tp", None)
    return jax.shard_map(
        step,
        mesh=mesh,
        in_specs=(tokens, tokens, P("dp", "tp"), P("dp", "tp"), columns, columns, rows),
        out_specs=(tokens, P("dp", "tp"), P("dp", "tp"), P(("dp", "tp"), None)),
        check_vma=False,
    )
```

```python
import functools

import jax
import jax.numpy as jnp
from jax import lax
from jax.experimental import pallas as pl
from jax.experimental.pallas import tpu as pltpu
from jax.sharding import PartitionSpec as P

MESH = pl.DeviceIdType.MESH
BF = jnp.bfloat16
F32 = jnp.float32
T = 256
NC = 8
D = 2048
F = 640
B = 128
L1, L2, L3, L4, L5 = 2, 2, 5, 8, 11
VIA = NC - 1
C0 = 0.7978845608028654
C1 = 0.044715


def dot(a, b, dims=((1,), (0,))):
    return lax.dot_general(a, b, (dims, ((), ())), preferred_element_type=F32)


def kernel(
    x_hbm, dy_hbm, gate_hbm, up_hbm, wg_hbm, wu_hbm, wd_hbm,
    dx, dwg, dwu, dwd,
    wcat, wd, dcat, hid, dyc, guc, pan, dh, act_s, slope_s, keep, outs,
    c1s, c1r, p1s, p1r, p2s, p2r, extra,
    dy_sem, gu_sem, wd_sem, w_sem, pan_sem,
    c1_sem, p1_sem, p2_sem, cf_sem, sent, extra_sem,
):
    me = lax.axis_index("tp")
    c = lax.rem(me, 2)
    y = lax.rem(me // 2, 2)
    x = me // 4
    nx, ny, nc = me + 4 - 8 * x, me + 2 - 4 * y, me + 1 - 2 * c
    first_chip, last_chip = x + y == 0, x + y == 2

    barrier = pltpu.get_barrier_semaphore()
    for to in (nx, ny, nc):
        pl.semaphore_signal(barrier, inc=1, device_id={"tp": to}, device_id_type=MESH)

    def rcopy(src, dst, ss, rs, to):
        return pltpu.make_async_remote_copy(
            src_ref=src, dst_ref=dst, send_sem=ss, recv_sem=rs, device_id={"tp": to}, device_id_type=MESH
        )

    def take(ref, sem):
        pltpu.make_async_copy(ref, ref, sem).wait()

    def load_gu(k, s):
        rows = pl.ds(pl.multiple_of(k * T, T), T)
        pltpu.make_async_copy(gate_hbm.at[rows], guc.at[s, 0], gu_sem.at[s]).start()
        pltpu.make_async_copy(up_hbm.at[rows], guc.at[s, 1], gu_sem.at[s]).start()

    def load_chunk(k, s):
        rows = pl.ds(pl.multiple_of(k * T, T), T)
        pltpu.make_async_copy(dy_hbm.at[rows], dyc.at[s], dy_sem.at[s]).start()
        load_gu(k, s)

    def load_panel(m, s):
        cols = pl.ds(pl.multiple_of(m * T, T), T)
        pltpu.make_async_copy(x_hbm.at[:, cols], pan.at[s, 0], pan_sem.at[s]).start()
        pltpu.make_async_copy(dy_hbm.at[:, cols], pan.at[s, 1], pan_sem.at[s]).start()

    def load_w(g):
        own, kept = g % 2, g // 2
        h = c if own else 1 - c
        for ab in range(2):
            first, second = (x, y) if ab == 0 else (y, x)
            i = first if kept else 1 - first
            for jo in range(2):
                j = second if jo else 1 - second
                src = pl.ds(pl.multiple_of(h * 1024 + ab * 512 + i * 256 + j * 128, B), B)
                dst = pl.ds((g * 4 + jo * 2 + ab) * B, B)
                pltpu.make_async_copy(wg_hbm.at[src], wcat.at[dst, 0:F], w_sem.at[g]).start()
                pltpu.make_async_copy(wu_hbm.at[src], wcat.at[dst, F : 2 * F], w_sem.at[g]).start()

    def piece(ref, k, ab, cx, cy, h):
        col = h * 1024 + (cx * 256 + cy * 128 if ab == 0 else 512 + cy * 256 + cx * 128)
        return ref.at[pl.ds(pl.multiple_of(k * T, T), T), pl.ds(pl.multiple_of(col, B), B)]

    def c1_part(ref, k, part):
        return ref.at[k, 1] if part == 2 else ref.at[k, 0, pl.ds(part * 256, 256)]

    def c1_send(k, part):
        rcopy(c1_part(c1s, k, part), c1_part(c1r, k, part), sent.at[0], c1_sem.at[lax.rem(k, 4), part], nc).start()

    def g_send(k, ab, kind):
        far, near = (ny, nx) if ab else (nx, ny)
        if kind == 2:
            ref = piece(dx, k, ab, x, 1 - y, c) if ab == 0 else piece(dx, k, ab, 1 - x, y, c)
        else:
            ref = piece(dx, k, ab, x, y, c)
        rcopy(ref, ref, sent.at[3], (p2_sem if kind == 2 else p1_sem).at[k], near if kind == 0 else far).start()

    def cf_send(k, ab, which):
        cx, cy = ((x, y), (x, 1 - y), (1 - x, y), (1 - x, 1 - y))[which]
        ref = piece(dx, k, ab, cx, cy, c)
        rcopy(ref, ref, sent.at[4], cf_sem, nc).start()

    def s1(k, jo):
        with jax.named_scope("s1"):
            take(c1_part(c1r, k, jo), c1_sem.at[lax.rem(k, 4), jo])
        for ab in range(2):
            rows = pl.ds(jo * 256 + ab * B, B)
            p1s[k, jo, ab] = (outs[rows] + c1r[k, 0, rows].astype(F32)).astype(BF)
            across, other = (ny, nx) if ab else (nx, ny)
            plain = rcopy(p1s.at[k, jo, ab], p1r.at[k, jo, ab], sent.at[1], p1_sem.at[k], across)
            if jo:
                skip = jnp.logical_and(k == VIA, last_chip)
            else:
                skip = jnp.logical_and(k == VIA, jnp.logical_and(x + y == 1, (y if ab else x) == 1))

                @pl.when(skip)
                def _():
                    rcopy(p1s.at[k, jo, ab], extra.at[ab], sent.at[1], extra_sem, other).start()

            pl.when(jnp.logical_not(skip))(plain.start)

    def s1_late():
        @pl.when(last_chip)
        def _():
            with jax.named_scope("late"):
                take(extra, extra_sem)
            for ab in range(2):
                rows = pl.ds(256 + ab * B, B)
                total = outs[rows] + c1r[VIA, 0, rows].astype(F32) + extra[ab].astype(F32)
                p1s[VIA, 1, ab] = total.astype(BF)
                rcopy(
                    p1s.at[VIA, 1, ab], p1r.at[VIA, 1, ab], sent.at[1], p1_sem.at[VIA], ny if ab else nx
                ).start()

    def s2(k):
        with jax.named_scope("s2"):
            take(c1r.at[k, 1], c1_sem.at[lax.rem(k, 4), 2])
        alone = jnp.logical_and(k == VIA, first_chip)

        def total(jo, ab):
            rows = pl.ds(jo * 256 + ab * B, B)
            return keep[k, rows] + c1r[k, 1, rows].astype(F32)

        def send(ab):
            rcopy(p2s.at[k, ab], p2r.at[k, ab], sent.at[2], p2_sem.at[k], nx if ab else ny).start()

        @pl.when(alone)
        def _():
            take(p1r.at[k, 1], p1_sem.at[k])
            for ab in range(2):
                p2s[k, ab] = total(0, ab).astype(BF)
                send(ab)

        @pl.when(jnp.logical_not(alone))
        def _():
            with jax.named_scope("s2"):
                take(p1r.at[k], p1_sem.at[k])
            for ab in range(2):
                p2s[k, ab] = (total(0, ab) + p1r[k, 0, ab].astype(F32)).astype(BF)
                send(ab)

        for ab in range(2):
            keep[k, pl.ds(256 + ab * B, B)] = total(1, ab) + p1r[k, 1, ab].astype(F32)

    @jax.named_scope("s3")
    def s3(k):
        take(p2r.at[k], p2_sem.at[k])
        for ab in range(2):
            done = (keep[k, pl.ds(256 + ab * B, B)] + p2r[k, ab].astype(F32)).astype(BF)
            piece(dx, k, ab, x, y, c)[...] = done.T
            g_send(k, ab, 0)
            g_send(k, ab, 1)
            cf_send(k, ab, 0)

    @jax.named_scope("s4")
    def s4(k):
        take(p1r.at[k], p1_sem.at[k])
        for ab in range(2):
            g_send(k, ab, 2)
            cf_send(k, ab, 1)
            cf_send(k, ab, 2)

    @jax.named_scope("s5")
    def s5(k):
        take(p2r.at[k], p2_sem.at[k])
        for ab in range(2):
            cf_send(k, ab, 3)

    def exchange(k, lag, fn):
        @pl.when(jnp.logical_and(k >= lag, k < NC + lag))
        def _():
            fn(k - lag)

    def gates(k, slot):
        cols = pl.ds(pl.multiple_of(k * T, T), T)
        for r in range(5):
            rows = slice(r * B, (r + 1) * B)
            g = guc[slot, 0, :, rows].T.astype(F32)
            u = guc[slot, 1, :, rows].T.astype(F32)
            g2 = g * g
            t = jnp.tanh(g * (C0 + (C0 * C1) * g2))
            cdf = 0.5 + 0.5 * t
            act = g * cdf
            slope = cdf + (act * (1.0 - t)) * (C0 + (3.0 * C0 * C1) * g2)
            hid[rows, cols] = (act * u).astype(BF)
            act_s[rows] = act
            slope_s[rows] = u * slope

    def store_grads(k, r, d):
        cols = pl.ds(pl.multiple_of(k * T, T), T)
        dcat[r, cols] = (d * slope_s[r]).astype(BF)
        dcat[F + r.start : F + r.stop, cols] = (d * act_s[r]).astype(BF)

    def halves(n):
        return [slice(i * n // 2, (i + 1) * n // 2) for i in range(2)]

    def term(k, rows):
        return dot(wcat[rows], dcat[:, pl.ds(pl.multiple_of(k * T, T), T)])

    parts = halves(D)

    def load_first(i):
        d = parts[i]
        pltpu.make_async_copy(wd_hbm.at[:, d], wd.at[:, d], wd_sem.at[i]).start()
        pltpu.make_async_copy(dy_hbm.at[0:T, d], dyc.at[0, :, d], wd_sem.at[2 + i]).start()

    def grads(k, slot, i, gated=False):
        with jax.named_scope("grads"):
            if not i and not gated:
                gates(k, slot)
            for r in halves(F):
                part = dot(wd[r, parts[i]], dyc[slot, :, parts[i]], ((1,), (1,)))
                if i:
                    store_grads(k, r, dh[r] + part)
                else:
                    dh[r] = part

    load_gu(0, 0)
    load_first(0)
    pl.delay(250)
    load_first(1)
    pl.delay(250)
    load_w(0)
    with jax.named_scope("load"):
        take(guc.at[0], gu_sem.at[0])
    with jax.named_scope("gates"):
        gates(0, 0)
    for i, d in enumerate(parts):
        with jax.named_scope("load"):
            take(wd.at[:, d], wd_sem.at[i])
            take(dyc.at[0, :, d], wd_sem.at[2 + i])
        if not i:
            load_w(1)
            load_chunk(1, 1)
        grads(0, 0, i, gated=True)
    load_w(2)
    load_w(3)
    with jax.named_scope("bar"):
        pl.semaphore_wait(barrier, 3)

    def first_use(k, g):
        @pl.when(k == 0)
        def _():
            take(wcat.at[g * 512 : (g + 1) * 512], w_sem.at[g])

    def keep_partner(k):
        first_use(k, 2)
        with jax.named_scope("keeps"):
            for r in halves(512):
                c1s[k, 1, r] = term(k, slice(1024 + r.start, 1024 + r.stop)).astype(BF)
        c1_send(k, 2)

    def keep_own(k):
        first_use(k, 3)
        with jax.named_scope("keeps"):
            for r in halves(512):
                keep[k, r] = term(k, slice(1536 + r.start, 1536 + r.stop))

    def phase1(k, _):
        first_use(k, 0)
        for ab in range(2):
            with jax.named_scope("termP"):
                for i in range(2):
                    r = slice(ab * 256 + i * 128, ab * 256 + (i + 1) * 128)
                    c1s[k, 0, r] = term(k, r).astype(BF)
            c1_send(k, ab)
        first_use(k, 1)
        with jax.named_scope("out"):
            for r in halves(512):
                outs[r] = term(k, slice(512 + r.start, 512 + r.stop))
        s1(k, 0)

        @pl.when(k >= L1)
        def _():
            keep_partner(k - L1)

        nxt = k + 1
        slot = lax.rem(nxt, 2)

        @pl.when(k < NC - 1)
        def _():
            take(dyc.at[slot], dy_sem.at[slot])
            take(guc.at[slot], gu_sem.at[slot])
            grads(nxt, slot, 0)

        s1(k, 1)

        @pl.when(k >= L1)
        def _():
            keep_own(k - L1)

        @pl.when(k < NC - 1)
        def _():
            @pl.when(nxt < NC - 1)
            def _():
                load_chunk(nxt + 1, 1 - slot)

            @pl.when(jnp.logical_and(k >= 2, k < 4))
            def _():
                load_panel(k - 2, k - 2)

            grads(nxt, slot, 1)

        exchange(k, L2, s2)
        exchange(k, L3, s3)
        exchange(k, L4, s4)
        exchange(k, L5, s5)
        return 0

    lax.fori_loop(0, NC, phase1, 0)

    def last_keeps(k, _):
        keep_partner(k)
        keep_own(k)
        return 0

    lax.fori_loop(NC - L1, NC, last_keeps, 0)

    def phase2(m, _):
        slot = lax.rem(m, 2)
        k = NC + m
        at = pl.ds(pl.multiple_of(m * T, T), T)
        take(pan.at[slot], pan_sem.at[slot])
        with jax.named_scope("dwg"):
            for r in halves(F):
                dwg[at, r] = dot(dcat[r], pan[slot, 0]).astype(BF).T
        pl.when(m == 0)(s1_late)
        exchange(k, L2, s2)
        with jax.named_scope("dwu"):
            for r in halves(F):
                dwu[at, r] = dot(dcat[F + r.start : F + r.stop], pan[slot, 0]).astype(BF).T
        exchange(k, L3, s3)
        exchange(k, L4, s4)
        with jax.named_scope("dwd"):
            for r in halves(F):
                dwd[r, at] = dot(hid[r], pan[slot, 1]).astype(BF)

        @pl.when(m < NC - 2)
        def _():
            load_panel(m + 2, slot)

        exchange(k, L5, s5)
        return 0

    lax.fori_loop(0, NC, phase2, 0)

    def phase3(k, _):
        exchange(k, L4, s4)
        exchange(k, L5, s5)
        return 0

    lax.fori_loop(2 * NC, NC + L5, phase3, 0)
    with jax.named_scope("fin"):
        for i, ref in enumerate((c1s, p1s, p2s, dx.at[0:768], dx.at[0:1024])):
            take(ref, sent.at[i])
        take(c1r, cf_sem)


def write_out(dx, dwg, dwu, dwd, dx_o, dwg_o, dwu_o, dwd_o, sem):
    copies = []
    for src, dst, parts in ((dx, dx_o, 4), (dwg, dwg_o, 2), (dwu, dwu_o, 2), (dwd, dwd_o, 2)):
        n = src.shape[0] // parts
        for i in range(parts):
            rows = pl.ds(i * n, n)
            copies.append(pltpu.make_async_copy(src.at[rows], dst.at[rows], sem.at[len(copies)]))
    for cp in copies:
        cp.start()
    for cp in copies:
        cp.wait()


def solution(mesh):
    def step(x, dy, gate, up, w_gate, w_up, w_down):
        hbm = pl.BlockSpec(memory_space=pltpu.HBM)
        vmem = pl.BlockSpec(memory_space=pltpu.VMEM)
        shapes = ((D, D), (D, F), (D, F), (F, D))
        dma = pltpu.SemaphoreType.DMA
        args = [pltpu.with_memory_space_constraint(a, pltpu.HBM) for a in (x, dy, gate, up, w_gate, w_up, w_down)]
        results = pl.pallas_call(
            kernel,
            out_shape=tuple(pltpu.VMEM(s, BF) for s in shapes),
            in_specs=[hbm] * 7,
            out_specs=(vmem,) * 4,
            scratch_shapes=[
                pltpu.VMEM((D, 2 * F), BF),
                pltpu.VMEM((F, D), BF),
                pltpu.VMEM((2 * F, D), BF),
                pltpu.VMEM((F, D), BF),
                pltpu.VMEM((2, T, D), BF),
                pltpu.VMEM((2, 2, T, F), BF),
                pltpu.VMEM((2, 2, D, T), BF),
                pltpu.VMEM((F, T), F32),
                pltpu.VMEM((F, T), F32),
                pltpu.VMEM((F, T), F32),
                pltpu.VMEM((NC, 512, T), F32),
                pltpu.VMEM((512, T), F32),
                pltpu.VMEM((NC, 2, 512, T), BF),
                pltpu.VMEM((NC, 2, 512, T), BF),
                pltpu.VMEM((NC, 2, 2, B, T), BF),
                pltpu.VMEM((NC, 2, 2, B, T), BF),
                pltpu.VMEM((NC, 2, 128, T), BF),
                pltpu.VMEM((NC, 2, 128, T), BF),
                pltpu.VMEM((2, 128, T), BF),
                dma((2,)),
                dma((2,)),
                dma((4,)),
                dma((4,)),
                dma((2,)),
                dma((4, 3)),
                dma((NC,)),
                dma((NC,)),
                dma,
                dma((5,)),
                dma,
            ],
            compiler_params=pltpu.CompilerParams(
                collective_id=0, has_side_effects=True, vmem_limit_bytes=48 * 2**20
            ),
        )(*args)
        return pl.pallas_call(
            write_out,
            out_shape=tuple(jax.ShapeDtypeStruct(s, BF) for s in shapes),
            in_specs=[vmem] * 4,
            out_specs=(hbm,) * 4,
            scratch_shapes=[dma((10,))],
            compiler_params=pltpu.CompilerParams(vmem_limit_bytes=2**20),
        )(*results)

    tokens, columns, rows = P("dp", None), P(None, "tp"), P("tp", None)
    return jax.shard_map(
        step,
        mesh=mesh,
        in_specs=(tokens, tokens, P("dp", "tp"), P("dp", "tp"), columns, columns, rows),
        out_specs=(tokens, P("dp", "tp"), P("dp", "tp"), P(("dp", "tp"), None)),
        check_vma=False,
    )
```

```python
import functools

import jax
import jax.numpy as jnp
from jax import lax
from jax.experimental import pallas as pl
from jax.experimental.pallas import tpu as pltpu
from jax.sharding import PartitionSpec as P

MESH = pl.DeviceIdType.MESH
BF = jnp.bfloat16
F32 = jnp.float32
T = 256
NC = 8
D = 2048
F = 640
B = 128
L1, L2, L3, L4, L5 = 2, 2, 5, 8, 11
VIA = NC - 1
C0 = 0.7978845608028654
C1 = 0.044715


def dot(a, b, dims=((1,), (0,))):
    return lax.dot_general(a, b, (dims, ((), ())), preferred_element_type=F32)


def kernel(
    x_hbm, dy_hbm, gate_hbm, up_hbm, wg_hbm, wu_hbm, wd_hbm,
    dx, dwg, dwu, dwd,
    wcat, wd, dcat, hid, dyc, guc, pan, dh, act_s, slope_s, keep, outs,
    c1s, c1r, p1s, p1r, p2s, p2r, extra,
    dy_sem, gu_sem, wd_sem, w_sem, pan_sem,
    c1_sem, p1_sem, p2_sem, cf_sem, sent, extra_sem,
):
    me = lax.axis_index("tp")
    c = lax.rem(me, 2)
    y = lax.rem(me // 2, 2)
    x = me // 4
    nx, ny, nc = me + 4 - 8 * x, me + 2 - 4 * y, me + 1 - 2 * c
    first_chip, last_chip = x + y == 0, x + y == 2

    barrier = pltpu.get_barrier_semaphore()
    for to in (nx, ny, nc):
        pl.semaphore_signal(barrier, inc=1, device_id={"tp": to}, device_id_type=MESH)

    def rcopy(src, dst, ss, rs, to):
        return pltpu.make_async_remote_copy(
            src_ref=src, dst_ref=dst, send_sem=ss, recv_sem=rs, device_id={"tp": to}, device_id_type=MESH
        )

    def take(ref, sem):
        pltpu.make_async_copy(ref, ref, sem).wait()

    def load_gu(k, s):
        rows = pl.ds(pl.multiple_of(k * T, T), T)
        pltpu.make_async_copy(gate_hbm.at[rows], guc.at[s, 0], gu_sem.at[s]).start()
        pltpu.make_async_copy(up_hbm.at[rows], guc.at[s, 1], gu_sem.at[s]).start()

    def load_chunk(k, s):
        rows = pl.ds(pl.multiple_of(k * T, T), T)
        pltpu.make_async_copy(dy_hbm.at[rows], dyc.at[s], dy_sem.at[s]).start()
        load_gu(k, s)

    def load_panel(m, s):
        cols = pl.ds(pl.multiple_of(m * T, T), T)
        pltpu.make_async_copy(x_hbm.at[:, cols], pan.at[s, 0], pan_sem.at[s]).start()
        pltpu.make_async_copy(dy_hbm.at[:, cols], pan.at[s, 1], pan_sem.at[s]).start()

    def load_w(g):
        own, kept = g % 2, g // 2
        h = c if own else 1 - c
        for ab in range(2):
            first, second = (x, y) if ab == 0 else (y, x)
            i = first if kept else 1 - first
            for jo in range(2):
                j = second if jo else 1 - second
                src = pl.ds(pl.multiple_of(h * 1024 + ab * 512 + i * 256 + j * 128, B), B)
                dst = pl.ds((g * 4 + jo * 2 + ab) * B, B)
                pltpu.make_async_copy(wg_hbm.at[src], wcat.at[dst, 0:F], w_sem.at[g]).start()
                pltpu.make_async_copy(wu_hbm.at[src], wcat.at[dst, F : 2 * F], w_sem.at[g]).start()

    def piece(ref, k, ab, cx, cy, h):
        col = h * 1024 + (cx * 256 + cy * 128 if ab == 0 else 512 + cy * 256 + cx * 128)
        return ref.at[pl.ds(pl.multiple_of(k * T, T), T), pl.ds(pl.multiple_of(col, B), B)]

    def c1_part(ref, k, part):
        return ref.at[k, 1] if part == 2 else ref.at[k, 0, pl.ds(part * 256, 256)]

    def c1_send(k, part):
        rcopy(c1_part(c1s, k, part), c1_part(c1r, k, part), sent.at[0], c1_sem.at[lax.rem(k, 4), part], nc).start()

    def g_send(k, ab, kind):
        far, near = (ny, nx) if ab else (nx, ny)
        if kind == 2:
            ref = piece(dx, k, ab, x, 1 - y, c) if ab == 0 else piece(dx, k, ab, 1 - x, y, c)
        else:
            ref = piece(dx, k, ab, x, y, c)
        rcopy(ref, ref, sent.at[3], (p2_sem if kind == 2 else p1_sem).at[k], near if kind == 0 else far).start()

    def cf_send(k, ab, which):
        cx, cy = ((x, y), (x, 1 - y), (1 - x, y), (1 - x, 1 - y))[which]
        ref = piece(dx, k, ab, cx, cy, c)
        rcopy(ref, ref, sent.at[4], cf_sem, nc).start()

    def s1(k, jo):
        with jax.named_scope("s1"):
            take(c1_part(c1r, k, jo), c1_sem.at[lax.rem(k, 4), jo])
        for ab in range(2):
            rows = pl.ds(jo * 256 + ab * B, B)
            p1s[k, jo, ab] = (outs[rows] + c1r[k, 0, rows].astype(F32)).astype(BF)
            across, other = (ny, nx) if ab else (nx, ny)
            plain = rcopy(p1s.at[k, jo, ab], p1r.at[k, jo, ab], sent.at[1], p1_sem.at[k], across)
            if jo:
                skip = jnp.logical_and(k == VIA, last_chip)
            else:
                skip = jnp.logical_and(k == VIA, jnp.logical_and(x + y == 1, (y if ab else x) == 1))

                @pl.when(skip)
                def _():
                    rcopy(p1s.at[k, jo, ab], extra.at[ab], sent.at[1], extra_sem, other).start()

            pl.when(jnp.logical_not(skip))(plain.start)

    def s1_late():
        @pl.when(last_chip)
        def _():
            with jax.named_scope("late"):
                take(extra, extra_sem)
            for ab in range(2):
                rows = pl.ds(256 + ab * B, B)
                total = outs[rows] + c1r[VIA, 0, rows].astype(F32) + extra[ab].astype(F32)
                p1s[VIA, 1, ab] = total.astype(BF)
                rcopy(
                    p1s.at[VIA, 1, ab], p1r.at[VIA, 1, ab], sent.at[1], p1_sem.at[VIA], ny if ab else nx
                ).start()

    def s2(k):
        with jax.named_scope("s2"):
            take(c1r.at[k, 1], c1_sem.at[lax.rem(k, 4), 2])
        alone = jnp.logical_and(k == VIA, first_chip)

        def total(jo, ab):
            rows = pl.ds(jo * 256 + ab * B, B)
            return keep[k, rows] + c1r[k, 1, rows].astype(F32)

        def send(ab):
            rcopy(p2s.at[k, ab], p2r.at[k, ab], sent.at[2], p2_sem.at[k], nx if ab else ny).start()

        @pl.when(alone)
        def _():
            take(p1r.at[k, 1], p1_sem.at[k])
            for ab in range(2):
                p2s[k, ab] = total(0, ab).astype(BF)
                send(ab)

        @pl.when(jnp.logical_not(alone))
        def _():
            with jax.named_scope("s2"):
                take(p1r.at[k], p1_sem.at[k])
            for ab in range(2):
                p2s[k, ab] = (total(0, ab) + p1r[k, 0, ab].astype(F32)).astype(BF)
                send(ab)

        for ab in range(2):
            keep[k, pl.ds(256 + ab * B, B)] = total(1, ab) + p1r[k, 1, ab].astype(F32)

    @jax.named_scope("s3")
    def s3(k):
        take(p2r.at[k], p2_sem.at[k])
        for ab in range(2):
            done = (keep[k, pl.ds(256 + ab * B, B)] + p2r[k, ab].astype(F32)).astype(BF)
            piece(dx, k, ab, x, y, c)[...] = done.T
            g_send(k, ab, 0)
            g_send(k, ab, 1)
            cf_send(k, ab, 0)

    @jax.named_scope("s4")
    def s4(k):
        take(p1r.at[k], p1_sem.at[k])
        for ab in range(2):
            g_send(k, ab, 2)
            cf_send(k, ab, 1)
            cf_send(k, ab, 2)

    @jax.named_scope("s5")
    def s5(k):
        take(p2r.at[k], p2_sem.at[k])
        for ab in range(2):
            cf_send(k, ab, 3)

    def exchange(k, lag, fn):
        @pl.when(jnp.logical_and(k >= lag, k < NC + lag))
        def _():
            fn(k - lag)

    def gates(k, slot):
        cols = pl.ds(pl.multiple_of(k * T, T), T)
        for r in range(5):
            rows = slice(r * B, (r + 1) * B)
            g = guc[slot, 0, :, rows].T.astype(F32)
            u = guc[slot, 1, :, rows].T.astype(F32)
            g2 = g * g
            t = jnp.tanh(g * (C0 + (C0 * C1) * g2))
            cdf = 0.5 + 0.5 * t
            act = g * cdf
            slope = cdf + (act * (1.0 - t)) * (C0 + (3.0 * C0 * C1) * g2)
            hid[rows, cols] = (act * u).astype(BF)
            act_s[rows] = act
            slope_s[rows] = u * slope

    def store_grads(k, r, d):
        cols = pl.ds(pl.multiple_of(k * T, T), T)
        dcat[r, cols] = (d * slope_s[r]).astype(BF)
        dcat[F + r.start : F + r.stop, cols] = (d * act_s[r]).astype(BF)

    def halves(n):
        return [slice(i * n // 2, (i + 1) * n // 2) for i in range(2)]

    def term(k, rows):
        return dot(wcat[rows], dcat[:, pl.ds(pl.multiple_of(k * T, T), T)])

    parts = (slice(0, 512), slice(512, 1280), slice(1280, D))

    def load_first(i):
        d = parts[i]
        pltpu.make_async_copy(wd_hbm.at[:, d], wd.at[:, d], wd_sem.at[i]).start()
        pltpu.make_async_copy(dy_hbm.at[0:T, d], dyc.at[0, :, d], wd_sem.at[3 + i]).start()

    def grads(k, slot, parts, i):
        with jax.named_scope("grads"):
            if not i:
                gates(k, slot)
            for r in halves(F):
                part = dot(wd[r, parts[i]], dyc[slot, :, parts[i]], ((1,), (1,)))
                total = dh[r] + part if i else part
                if i == len(parts) - 1:
                    store_grads(k, r, total)
                else:
                    dh[r] = total

    load_first(0)
    load_gu(0, 0)
    pl.delay(250)
    load_first(1)
    pl.delay(250)
    load_first(2)
    pl.delay(250)
    load_w(0)
    for i, d in enumerate(parts):
        with jax.named_scope("load"):
            if not i:
                take(guc.at[0], gu_sem.at[0])
            take(wd.at[:, d], wd_sem.at[i])
            take(dyc.at[0, :, d], wd_sem.at[3 + i])
        if not i:
            load_w(1)
            load_chunk(1, 1)
        grads(0, 0, parts, i)
    load_w(2)
    load_w(3)
    with jax.named_scope("bar"):
        pl.semaphore_wait(barrier, 3)

    def first_use(k, g):
        @pl.when(k == 0)
        def _():
            take(wcat.at[g * 512 : (g + 1) * 512], w_sem.at[g])

    def keep_partner(k):
        first_use(k, 2)
        with jax.named_scope("keeps"):
            for r in halves(512):
                c1s[k, 1, r] = term(k, slice(1024 + r.start, 1024 + r.stop)).astype(BF)
        c1_send(k, 2)

    def keep_own(k):
        first_use(k, 3)
        with jax.named_scope("keeps"):
            for r in halves(512):
                keep[k, r] = term(k, slice(1536 + r.start, 1536 + r.stop))

    def phase1(k, _):
        first_use(k, 0)
        for ab in range(2):
            with jax.named_scope("termP"):
                for i in range(2):
                    r = slice(ab * 256 + i * 128, ab * 256 + (i + 1) * 128)
                    c1s[k, 0, r] = term(k, r).astype(BF)
            c1_send(k, ab)
        first_use(k, 1)
        with jax.named_scope("out"):
            for r in halves(512):
                outs[r] = term(k, slice(512 + r.start, 512 + r.stop))
        s1(k, 0)

        @pl.when(k >= L1)
        def _():
            keep_partner(k - L1)

        nxt = k + 1
        slot = lax.rem(nxt, 2)

        @pl.when(k < NC - 1)
        def _():
            take(dyc.at[slot], dy_sem.at[slot])
            take(guc.at[slot], gu_sem.at[slot])
            grads(nxt, slot, halves(D), 0)

        s1(k, 1)

        @pl.when(k >= L1)
        def _():
            keep_own(k - L1)

        @pl.when(k < NC - 1)
        def _():
            @pl.when(nxt < NC - 1)
            def _():
                load_chunk(nxt + 1, 1 - slot)

            @pl.when(jnp.logical_and(k >= 2, k < 4))
            def _():
                load_panel(k - 2, k - 2)

            grads(nxt, slot, halves(D), 1)

        exchange(k, L2, s2)
        exchange(k, L3, s3)
        exchange(k, L4, s4)
        exchange(k, L5, s5)
        return 0

    lax.fori_loop(0, NC, phase1, 0)

    def last_keeps(k, _):
        keep_partner(k)
        keep_own(k)
        return 0

    lax.fori_loop(NC - L1, NC, last_keeps, 0)

    def phase2(m, _):
        slot = lax.rem(m, 2)
        k = NC + m
        at = pl.ds(pl.multiple_of(m * T, T), T)
        take(pan.at[slot], pan_sem.at[slot])
        with jax.named_scope("dwg"):
            for r in halves(F):
                dwg[at, r] = dot(dcat[r], pan[slot, 0]).astype(BF).T
        pl.when(m == 0)(s1_late)
        exchange(k, L2, s2)
        with jax.named_scope("dwu"):
            for r in halves(F):
                dwu[at, r] = dot(dcat[F + r.start : F + r.stop], pan[slot, 0]).astype(BF).T
        exchange(k, L3, s3)
        exchange(k, L4, s4)
        with jax.named_scope("dwd"):
            for r in halves(F):
                dwd[r, at] = dot(hid[r], pan[slot, 1]).astype(BF)

        @pl.when(m < NC - 2)
        def _():
            load_panel(m + 2, slot)

        exchange(k, L5, s5)
        return 0

    lax.fori_loop(0, NC, phase2, 0)

    def phase3(k, _):
        exchange(k, L4, s4)
        exchange(k, L5, s5)
        return 0

    lax.fori_loop(2 * NC, NC + L5, phase3, 0)
    with jax.named_scope("fin"):
        for i, ref in enumerate((c1s, p1s, p2s, dx.at[0:768], dx.at[0:1024])):
            take(ref, sent.at[i])
        take(c1r, cf_sem)


def write_out(dx, dwg, dwu, dwd, dx_o, dwg_o, dwu_o, dwd_o, sem):
    copies = []
    for src, dst, parts in ((dx, dx_o, 4), (dwg, dwg_o, 2), (dwu, dwu_o, 2), (dwd, dwd_o, 2)):
        n = src.shape[0] // parts
        for i in range(parts):
            rows = pl.ds(i * n, n)
            copies.append(pltpu.make_async_copy(src.at[rows], dst.at[rows], sem.at[len(copies)]))
    for cp in copies:
        cp.start()
    for cp in copies:
        cp.wait()


def solution(mesh):
    def step(x, dy, gate, up, w_gate, w_up, w_down):
        hbm = pl.BlockSpec(memory_space=pltpu.HBM)
        vmem = pl.BlockSpec(memory_space=pltpu.VMEM)
        shapes = ((D, D), (D, F), (D, F), (F, D))
        dma = pltpu.SemaphoreType.DMA
        args = [pltpu.with_memory_space_constraint(a, pltpu.HBM) for a in (x, dy, gate, up, w_gate, w_up, w_down)]
        results = pl.pallas_call(
            kernel,
            out_shape=tuple(pltpu.VMEM(s, BF) for s in shapes),
            in_specs=[hbm] * 7,
            out_specs=(vmem,) * 4,
            scratch_shapes=[
                pltpu.VMEM((D, 2 * F), BF),
                pltpu.VMEM((F, D), BF),
                pltpu.VMEM((2 * F, D), BF),
                pltpu.VMEM((F, D), BF),
                pltpu.VMEM((2, T, D), BF),
                pltpu.VMEM((2, 2, T, F), BF),
                pltpu.VMEM((2, 2, D, T), BF),
                pltpu.VMEM((F, T), F32),
                pltpu.VMEM((F, T), F32),
                pltpu.VMEM((F, T), F32),
                pltpu.VMEM((NC, 512, T), F32),
                pltpu.VMEM((512, T), F32),
                pltpu.VMEM((NC, 2, 512, T), BF),
                pltpu.VMEM((NC, 2, 512, T), BF),
                pltpu.VMEM((NC, 2, 2, B, T), BF),
                pltpu.VMEM((NC, 2, 2, B, T), BF),
                pltpu.VMEM((NC, 2, 128, T), BF),
                pltpu.VMEM((NC, 2, 128, T), BF),
                pltpu.VMEM((2, 128, T), BF),
                dma((2,)),
                dma((2,)),
                dma((6,)),
                dma((4,)),
                dma((2,)),
                dma((4, 3)),
                dma((NC,)),
                dma((NC,)),
                dma,
                dma((5,)),
                dma,
            ],
            compiler_params=pltpu.CompilerParams(
                collective_id=0, has_side_effects=True, vmem_limit_bytes=48 * 2**20
            ),
        )(*args)
        return pl.pallas_call(
            write_out,
            out_shape=tuple(jax.ShapeDtypeStruct(s, BF) for s in shapes),
            in_specs=[vmem] * 4,
            out_specs=(hbm,) * 4,
            scratch_shapes=[dma((10,))],
            compiler_params=pltpu.CompilerParams(vmem_limit_bytes=2**20),
        )(*results)

    tokens, columns, rows = P("dp", None), P(None, "tp"), P("tp", None)
    return jax.shard_map(
        step,
        mesh=mesh,
        in_specs=(tokens, tokens, P("dp", "tp"), P("dp", "tp"), columns, columns, rows),
        out_specs=(tokens, P("dp", "tp"), P("dp", "tp"), P(("dp", "tp"), None)),
        check_vma=False,
    )
```

```python
import functools

import jax
import jax.numpy as jnp
from jax import lax
from jax.experimental import pallas as pl
from jax.experimental.pallas import tpu as pltpu
from jax.sharding import PartitionSpec as P

MESH = pl.DeviceIdType.MESH
BF = jnp.bfloat16
F32 = jnp.float32
T = 256
NC = 8
D = 2048
F = 640
B = 128
L1, L2, L3, L4, L5 = 2, 2, 5, 8, 11
VIA = NC - 1
RV = 112
C0 = 0.7978845608028654
C1 = 0.044715


def dot(a, b, dims=((1,), (0,))):
    return lax.dot_general(a, b, (dims, ((), ())), preferred_element_type=F32)


def kernel(
    x_hbm, dy_hbm, gate_hbm, up_hbm, wg_hbm, wu_hbm, wd_hbm,
    dx, dwg, dwu, dwd,
    wcat, wd, dcat, hid, dyc, guc, pan, dh, act_s, slope_s, keep, outs,
    c1s, c1r, p1s, p1r, p2s, p2r, extra,
    in_sem, first_sem, w_sem, pan_sem,
    c1_sem, p1_sem, p2_sem, cf_sem, sent, extra_sem,
):
    me = lax.axis_index("tp")
    c = lax.rem(me, 2)
    y = lax.rem(me // 2, 2)
    x = me // 4
    nx, ny, nc = me + 4 - 8 * x, me + 2 - 4 * y, me + 1 - 2 * c
    first_chip, last_chip = x + y == 0, x + y == 2

    barrier = pltpu.get_barrier_semaphore()
    for to in (nx, ny, nc):
        pl.semaphore_signal(barrier, inc=1, device_id={"tp": to}, device_id_type=MESH)

    def rcopy(src, dst, ss, rs, to):
        return pltpu.make_async_remote_copy(
            src_ref=src, dst_ref=dst, send_sem=ss, recv_sem=rs, device_id={"tp": to}, device_id_type=MESH
        )

    def take(ref, sem):
        pltpu.make_async_copy(ref, ref, sem).wait()

    def load_gu(k, s, sem):
        rows = pl.ds(pl.multiple_of(k * T, T), T)
        pltpu.make_async_copy(gate_hbm.at[rows], guc.at[s, 0], sem).start()
        pltpu.make_async_copy(up_hbm.at[rows], guc.at[s, 1], sem).start()

    def load_chunk(k, s):
        rows = pl.ds(pl.multiple_of(k * T, T), T)
        pltpu.make_async_copy(dy_hbm.at[rows], dyc.at[s], in_sem.at[s]).start()
        load_gu(k, s, in_sem.at[s])

    def load_panel(m, s):
        cols = pl.ds(pl.multiple_of(m * T, T), T)
        pltpu.make_async_copy(x_hbm.at[:, cols], pan.at[s, 0], pan_sem.at[s]).start()
        pltpu.make_async_copy(dy_hbm.at[:, cols], pan.at[s, 1], pan_sem.at[s]).start()

    def load_w(g):
        own, kept = g % 2, g // 2
        h = c if own else 1 - c
        for ab in range(2):
            first, second = (x, y) if ab == 0 else (y, x)
            i = first if kept else 1 - first
            for jo in range(2):
                j = second if jo else 1 - second
                src = pl.ds(pl.multiple_of(h * 1024 + ab * 512 + i * 256 + j * 128, B), B)
                dst = pl.ds((g * 4 + jo * 2 + ab) * B, B)
                pltpu.make_async_copy(wg_hbm.at[src], wcat.at[dst, 0:F], w_sem.at[min(g, 2)]).start()
                pltpu.make_async_copy(wu_hbm.at[src], wcat.at[dst, F : 2 * F], w_sem.at[min(g, 2)]).start()

    def piece(ref, k, ab, cx, cy, h):
        col = h * 1024 + (cx * 256 + cy * 128 if ab == 0 else 512 + cy * 256 + cx * 128)
        return ref.at[pl.ds(pl.multiple_of(k * T, T), T), pl.ds(pl.multiple_of(col, B), B)]

    def c1_part(ref, k, part):
        return ref.at[k, 1] if part == 2 else ref.at[k, 0, pl.ds(part * 256, 256)]

    def c1_slot(k, part):
        return 4 + lax.rem(k, 4) if part == 2 else 2 * part + lax.rem(k, 2)

    def c1_send(k, part):
        rcopy(c1_part(c1s, k, part), c1_part(c1r, k, part), sent.at[1], c1_sem.at[c1_slot(k, part)], nc).start()

    def g_send(k, ab, kind):
        far, near = (ny, nx) if ab else (nx, ny)
        if kind == 2:
            ref = piece(dx, k, ab, x, 1 - y, c) if ab == 0 else piece(dx, k, ab, 1 - x, y, c)
        else:
            ref = piece(dx, k, ab, x, y, c)
        rcopy(ref, ref, sent.at[0], (p2_sem if kind == 2 else p1_sem).at[k], near if kind == 0 else far).start()

    def cf_send(k, ab, which):
        cx, cy = ((x, y), (x, 1 - y), (1 - x, y), (1 - x, 1 - y))[which]
        ref = piece(dx, k, ab, cx, cy, c)
        rcopy(ref, ref, sent.at[1], cf_sem, nc).start()

    def s1(k, jo):
        with jax.named_scope("s1"):
            take(c1_part(c1r, k, jo), c1_sem.at[c1_slot(k, jo)])
        for ab in range(2):
            rows = pl.ds(jo * 256 + ab * B, B)
            p1s[k, jo, ab] = (outs[rows] + c1r[k, 0, rows].astype(F32)).astype(BF)
            across, other = (ny, nx) if ab else (nx, ny)
            plain = rcopy(p1s.at[k, jo, ab], p1r.at[k, jo, ab], sent.at[0], p1_sem.at[k], across)
            if jo:
                skip = jnp.logical_and(k == VIA, last_chip)
            else:
                skip = jnp.logical_and(k == VIA, jnp.logical_and(x + y == 1, (y if ab else x) == 1))

                @pl.when(skip)
                def _():
                    part = p1s.at[k, jo, ab, pl.ds(0, RV)]
                    rcopy(part, extra.at[ab], sent.at[0], extra_sem, other).start()
                    rest = pl.ds(RV, B - RV)
                    src, dst = p1s.at[k, jo, ab, rest], p1r.at[k, jo, ab, rest]
                    rcopy(src, dst, sent.at[0], p1_sem.at[k], across).start()

            pl.when(jnp.logical_not(skip))(plain.start)

    def s1_late():
        @pl.when(last_chip)
        def _():
            with jax.named_scope("late"):
                take(extra, extra_sem)
            for ab in range(2):
                rows = pl.ds(256 + ab * B, RV)
                total = outs[rows] + c1r[VIA, 0, rows].astype(F32) + extra[ab].astype(F32)
                p1s[VIA, 1, ab, 0:RV] = total.astype(BF)
                rcopy(
                    p1s.at[VIA, 1, ab], p1r.at[VIA, 1, ab], sent.at[0], p1_sem.at[VIA], ny if ab else nx
                ).start()

    def s2(k):
        with jax.named_scope("s2"):
            take(c1r.at[k, 1], c1_sem.at[c1_slot(k, 2)])
        alone = jnp.logical_and(k == VIA, first_chip)

        def total(jo, ab):
            rows = pl.ds(jo * 256 + ab * B, B)
            return keep[k, rows] + c1r[k, 1, rows].astype(F32)

        def send(ab):
            rcopy(p2s.at[k, ab], p2r.at[k, ab], sent.at[0], p2_sem.at[k], nx if ab else ny).start()

        @pl.when(alone)
        def _():
            take(dcat.at[0 : 2 * (2 * B - RV) * T // 1024, 0:1024], p1_sem.at[k])
            for ab in range(2):
                mine = total(0, ab)
                p2s[k, ab, 0:RV] = mine[0:RV].astype(BF)
                p2s[k, ab, RV:B] = (mine[RV:B] + p1r[k, 0, ab, RV:B].astype(F32)).astype(BF)
                send(ab)

        @pl.when(jnp.logical_not(alone))
        def _():
            with jax.named_scope("s2"):
                take(p1r.at[k], p1_sem.at[k])
            for ab in range(2):
                p2s[k, ab] = (total(0, ab) + p1r[k, 0, ab].astype(F32)).astype(BF)
                send(ab)

        for ab in range(2):
            keep[k, pl.ds(256 + ab * B, B)] = total(1, ab) + p1r[k, 1, ab].astype(F32)

    @jax.named_scope("s3")
    def s3(k):
        take(p2r.at[k], p2_sem.at[k])
        for ab in range(2):
            done = (keep[k, pl.ds(256 + ab * B, B)] + p2r[k, ab].astype(F32)).astype(BF)
            piece(dx, k, ab, x, y, c)[...] = done.T
            g_send(k, ab, 0)
            g_send(k, ab, 1)
            cf_send(k, ab, 0)

    @jax.named_scope("s4")
    def s4(k):
        take(p1r.at[k], p1_sem.at[k])
        for ab in range(2):
            g_send(k, ab, 2)
            cf_send(k, ab, 1)
            cf_send(k, ab, 2)

    @jax.named_scope("s5")
    def s5(k):
        take(p2r.at[k], p2_sem.at[k])
        for ab in range(2):
            cf_send(k, ab, 3)

    def exchange(k, lag, fn):
        @pl.when(jnp.logical_and(k >= lag, k < NC + lag))
        def _():
            fn(k - lag)

    def gates(k, slot):
        cols = pl.ds(pl.multiple_of(k * T, T), T)
        for r in range(5):
            rows = slice(r * B, (r + 1) * B)
            g = guc[slot, 0, :, rows].T.astype(F32)
            u = guc[slot, 1, :, rows].T.astype(F32)
            g2 = g * g
            t = jnp.tanh(g * (C0 + (C0 * C1) * g2))
            cdf = 0.5 + 0.5 * t
            act = g * cdf
            slope = cdf + (act * (1.0 - t)) * (C0 + (3.0 * C0 * C1) * g2)
            hid[rows, cols] = (act * u).astype(BF)
            act_s[rows] = act
            slope_s[rows] = u * slope

    def store_grads(k, r, d):
        cols = pl.ds(pl.multiple_of(k * T, T), T)
        dcat[r, cols] = (d * slope_s[r]).astype(BF)
        dcat[F + r.start : F + r.stop, cols] = (d * act_s[r]).astype(BF)

    def halves(n):
        return [slice(i * n // 2, (i + 1) * n // 2) for i in range(2)]

    def term(k, rows):
        return dot(wcat[rows], dcat[:, pl.ds(pl.multiple_of(k * T, T), T)])

    parts = (slice(0, 512), slice(512, 1280), slice(1280, D))

    def load_first(i):
        d = parts[i]
        pltpu.make_async_copy(wd_hbm.at[:, d], wd.at[:, d], first_sem.at[i]).start()
        pltpu.make_async_copy(dy_hbm.at[0:T, d], dyc.at[0, :, d], first_sem.at[i]).start()

    def grads(k, slot, parts, i):
        with jax.named_scope("grads"):
            if not i:
                gates(k, slot)
            for r in halves(F):
                part = dot(wd[r, parts[i]], dyc[slot, :, parts[i]], ((1,), (1,)))
                total = dh[r] + part if i else part
                if i == len(parts) - 1:
                    store_grads(k, r, total)
                else:
                    dh[r] = total

    load_first(0)
    load_gu(0, 0, first_sem.at[0])
    pl.delay(250)
    load_first(1)
    pl.delay(250)
    load_first(2)
    pl.delay(250)
    load_w(0)
    for i, d in enumerate(parts):
        with jax.named_scope("load"):
            n = (T + F) * (d.stop - d.start) + (0 if i else 2 * T * F)
            take(dcat.at[0 : n // 1024, 0:1024], first_sem.at[i])
        if not i:
            load_w(1)
            load_chunk(1, 1)
        grads(0, 0, parts, i)
    load_w(2)
    load_w(3)
    with jax.named_scope("bar"):
        pl.semaphore_wait(barrier, 3)

    def first_use(k, g):
        @pl.when(k == 0)
        def _():
            take(wcat.at[g * 512 : 2048 if g == 2 else (g + 1) * 512], w_sem.at[g])

    def keep_partner(k):
        first_use(k, 2)
        with jax.named_scope("keeps"):
            for r in halves(512):
                c1s[k, 1, r] = term(k, slice(1024 + r.start, 1024 + r.stop)).astype(BF)
        c1_send(k, 2)

    def keep_own(k):
        with jax.named_scope("keeps"):
            for r in halves(512):
                keep[k, r] = term(k, slice(1536 + r.start, 1536 + r.stop))

    def phase1(k, _):
        first_use(k, 0)
        for ab in range(2):
            with jax.named_scope("termP"):
                for i in range(2):
                    r = slice(ab * 256 + i * 128, ab * 256 + (i + 1) * 128)
                    c1s[k, 0, r] = term(k, r).astype(BF)
            c1_send(k, ab)
        first_use(k, 1)
        with jax.named_scope("out"):
            for r in halves(512):
                outs[r] = term(k, slice(512 + r.start, 512 + r.stop))
        s1(k, 0)

        @pl.when(k >= L1)
        def _():
            keep_partner(k - L1)

        nxt = k + 1
        slot = lax.rem(nxt, 2)

        @pl.when(k < NC - 1)
        def _():
            take(dcat.at[0 : (T * D + 2 * T * F) // D], in_sem.at[slot])
            grads(nxt, slot, (slice(0, D),), 0)

            @pl.when(nxt < NC - 1)
            def _():
                load_chunk(nxt + 1, 1 - slot)

            @pl.when(jnp.logical_and(k >= 2, k < 4))
            def _():
                load_panel(k - 2, k - 2)

        s1(k, 1)

        @pl.when(k >= L1)
        def _():
            keep_own(k - L1)

        exchange(k, L2, s2)
        exchange(k, L3, s3)
        exchange(k, L4, s4)
        exchange(k, L5, s5)
        return 0

    lax.fori_loop(0, NC, phase1, 0)

    def last_keeps(k, _):
        keep_partner(k)
        keep_own(k)
        return 0

    lax.fori_loop(NC - L1, NC, last_keeps, 0)

    def phase2(m, _):
        slot = lax.rem(m, 2)
        k = NC + m
        at = pl.ds(pl.multiple_of(m * T, T), T)
        take(pan.at[slot], pan_sem.at[slot])
        with jax.named_scope("dwg"):
            for r in halves(F):
                dwg[at, r] = dot(dcat[r], pan[slot, 0]).astype(BF).T
        pl.when(m == 0)(s1_late)
        exchange(k, L2, s2)
        with jax.named_scope("dwu"):
            for r in halves(F):
                dwu[at, r] = dot(dcat[F + r.start : F + r.stop], pan[slot, 0]).astype(BF).T
        exchange(k, L3, s3)
        exchange(k, L4, s4)
        with jax.named_scope("dwd"):
            for r in halves(F):
                dwd[r, at] = dot(hid[r], pan[slot, 1]).astype(BF)

        @pl.when(m < NC - 2)
        def _():
            load_panel(m + 2, slot)

        exchange(k, L5, s5)
        return 0

    lax.fori_loop(0, NC, phase2, 0)

    def phase3(k, _):
        exchange(k, L4, s4)
        exchange(k, L5, s5)
        return 0

    lax.fori_loop(2 * NC, NC + L5, phase3, 0)
    with jax.named_scope("fin"):
        take(dx.at[0:1536], sent.at[0])
        take(dx, sent.at[1])
        take(c1r, cf_sem)


def write_out(dx, dwg, dwu, dwd, dx_o, dwg_o, dwu_o, dwd_o, sem):
    copies = []
    for src, dst, parts in ((dx, dx_o, 4), (dwg, dwg_o, 2), (dwu, dwu_o, 2), (dwd, dwd_o, 2)):
        n = src.shape[0] // parts
        for i in range(parts):
            rows = pl.ds(i * n, n)
            copies.append(pltpu.make_async_copy(src.at[rows], dst.at[rows], sem.at[len(copies)]))
    for cp in copies:
        cp.start()
    for cp in copies:
        cp.wait()


def solution(mesh):
    def step(x, dy, gate, up, w_gate, w_up, w_down):
        hbm = pl.BlockSpec(memory_space=pltpu.HBM)
        vmem = pl.BlockSpec(memory_space=pltpu.VMEM)
        shapes = ((D, D), (D, F), (D, F), (F, D))
        dma = pltpu.SemaphoreType.DMA
        args = [pltpu.with_memory_space_constraint(a, pltpu.HBM) for a in (x, dy, gate, up, w_gate, w_up, w_down)]
        results = pl.pallas_call(
            kernel,
            out_shape=tuple(pltpu.VMEM(s, BF) for s in shapes),
            in_specs=[hbm] * 7,
            out_specs=(vmem,) * 4,
            scratch_shapes=[
                pltpu.VMEM((D, 2 * F), BF),
                pltpu.VMEM((F, D), BF),
                pltpu.VMEM((2 * F, D), BF),
                pltpu.VMEM((F, D), BF),
                pltpu.VMEM((2, T, D), BF),
                pltpu.VMEM((2, 2, T, F), BF),
                pltpu.VMEM((2, 2, D, T), BF),
                pltpu.VMEM((F, T), F32),
                pltpu.VMEM((F, T), F32),
                pltpu.VMEM((F, T), F32),
                pltpu.VMEM((NC, 512, T), F32),
                pltpu.VMEM((512, T), F32),
                pltpu.VMEM((NC, 2, 512, T), BF),
                pltpu.VMEM((NC, 2, 512, T), BF),
                pltpu.VMEM((NC, 2, 2, B, T), BF),
                pltpu.VMEM((NC, 2, 2, B, T), BF),
                pltpu.VMEM((NC, 2, 128, T), BF),
                pltpu.VMEM((NC, 2, 128, T), BF),
                pltpu.VMEM((2, RV, T), BF),
                dma((2,)),
                dma((3,)),
                dma((3,)),
                dma((2,)),
                dma((8,)),
                dma((NC,)),
                dma((NC,)),
                dma,
                dma((2,)),
                dma,
            ],
            compiler_params=pltpu.CompilerParams(
                collective_id=0, has_side_effects=True, vmem_limit_bytes=48 * 2**20
            ),
        )(*args)
        return pl.pallas_call(
            write_out,
            out_shape=tuple(jax.ShapeDtypeStruct(s, BF) for s in shapes),
            in_specs=[vmem] * 4,
            out_specs=(hbm,) * 4,
            scratch_shapes=[dma((10,))],
            compiler_params=pltpu.CompilerParams(vmem_limit_bytes=2**20),
        )(*results)

    tokens, columns, rows = P("dp", None), P(None, "tp"), P("tp", None)
    return jax.shard_map(
        step,
        mesh=mesh,
        in_specs=(tokens, tokens, P("dp", "tp"), P("dp", "tp"), columns, columns, rows),
        out_specs=(tokens, P("dp", "tp"), P("dp", "tp"), P(("dp", "tp"), None)),
        check_vma=False,
    )
```

```python
import functools

import jax
import jax.numpy as jnp
from jax import lax
from jax.experimental import pallas as pl
from jax.experimental.pallas import tpu as pltpu
from jax.sharding import PartitionSpec as P

MESH = pl.DeviceIdType.MESH
BF = jnp.bfloat16
F32 = jnp.float32
T = 256
NC = 8
D = 2048
F = 640
B = 128
L1, L2, L3, L4, L5 = 2, 2, 5, 8, 11
VIA = NC - 1
RV = 112
C0 = 0.7978845608028654
C1 = 0.044715


def dot(a, b, dims=((1,), (0,))):
    return lax.dot_general(a, b, (dims, ((), ())), preferred_element_type=F32)


def kernel(
    x_hbm, dy_hbm, gate_hbm, up_hbm, wg_hbm, wu_hbm, wd_hbm,
    dx, dwg, dwu, dwd,
    wcat, wd, dcat, hid, dyc, guc, pan, dh, act_s, slope_s, keep, outs,
    c1s, c1r, p1s, p1r, p2s, p2r, extra,
    in_sem, first_sem, w_sem, pan_sem,
    c1_sem, p1_sem, p2_sem, cf_sem, sent, extra_sem, last_sem,
):
    me = lax.axis_index("tp")
    c = lax.rem(me, 2)
    y = lax.rem(me // 2, 2)
    x = me // 4
    nx, ny, nc = me + 4 - 8 * x, me + 2 - 4 * y, me + 1 - 2 * c
    first_chip, last_chip = x + y == 0, x + y == 2

    barrier = pltpu.get_barrier_semaphore()
    for to in (nx, ny, nc, nx + 1 - 2 * c, ny + 1 - 2 * c):
        pl.semaphore_signal(barrier, inc=1, device_id={"tp": to}, device_id_type=MESH)

    def rcopy(src, dst, ss, rs, to):
        return pltpu.make_async_remote_copy(
            src_ref=src, dst_ref=dst, send_sem=ss, recv_sem=rs, device_id={"tp": to}, device_id_type=MESH
        )

    def take(ref, sem):
        pltpu.make_async_copy(ref, ref, sem).wait()

    def load_gu(k, s, sem):
        rows = pl.ds(pl.multiple_of(k * T, T), T)
        pltpu.make_async_copy(gate_hbm.at[rows], guc.at[s, 0], sem).start()
        pltpu.make_async_copy(up_hbm.at[rows], guc.at[s, 1], sem).start()

    def load_chunk(k, s):
        rows = pl.ds(pl.multiple_of(k * T, T), T)
        pltpu.make_async_copy(dy_hbm.at[rows], dyc.at[s], in_sem.at[s]).start()
        load_gu(k, s, in_sem.at[s])

    def load_panel(m, s):
        cols = pl.ds(pl.multiple_of(m * T, T), T)
        pltpu.make_async_copy(x_hbm.at[:, cols], pan.at[s, 0], pan_sem.at[s]).start()
        pltpu.make_async_copy(dy_hbm.at[:, cols], pan.at[s, 1], pan_sem.at[s]).start()

    def load_w(g):
        own, kept = g % 2, g // 2
        h = c if own else 1 - c
        for ab in range(2):
            first, second = (x, y) if ab == 0 else (y, x)
            i = first if kept else 1 - first
            for jo in range(2):
                j = second if jo else 1 - second
                src = pl.ds(pl.multiple_of(h * 1024 + ab * 512 + i * 256 + j * 128, B), B)
                dst = pl.ds((g * 4 + jo * 2 + ab) * B, B)
                pltpu.make_async_copy(wg_hbm.at[src], wcat.at[dst, 0:F], w_sem.at[min(g, 2)]).start()
                pltpu.make_async_copy(wu_hbm.at[src], wcat.at[dst, F : 2 * F], w_sem.at[min(g, 2)]).start()

    def piece(ref, k, ab, cx, cy, h):
        col = h * 1024 + (cx * 256 + cy * 128 if ab == 0 else 512 + cy * 256 + cx * 128)
        return ref.at[pl.ds(pl.multiple_of(k * T, T), T), pl.ds(pl.multiple_of(col, B), B)]

    def c1_part(ref, k, part):
        return ref.at[k, 1] if part == 2 else ref.at[k, 0, pl.ds(part * 256, 256)]

    def c1_slot(k, part):
        return 4 + lax.rem(k, 4) if part == 2 else 2 * part + lax.rem(k, 2)

    def c1_send(k, part):
        rcopy(c1_part(c1s, k, part), c1_part(c1r, k, part), sent.at[1], c1_sem.at[c1_slot(k, part)], nc).start()

    def g_send(k, ab, kind):
        far, near = (ny, nx) if ab else (nx, ny)
        if kind == 2:
            ref = piece(dx, k, ab, x, 1 - y, c) if ab == 0 else piece(dx, k, ab, 1 - x, y, c)
        else:
            ref = piece(dx, k, ab, x, y, c)
        rcopy(ref, ref, sent.at[0], (p2_sem if kind == 2 else p1_sem).at[k], near if kind == 0 else far).start()

    def cf_send(k, ab, which, h=c, sem=1):
        cx, cy = ((x, y), (x, 1 - y), (1 - x, y), (1 - x, 1 - y))[which]
        ref = piece(dx, k, ab, cx, cy, h)
        rcopy(ref, ref, sent.at[sem], cf_sem, nc).start()

    def g_send_last(ab):
        cx, cy = (x, 1 - y) if ab == 0 else (1 - x, y)
        ref = piece(dx, NC - 1, ab, cx, cy, c)
        rcopy(ref, ref, sent.at[0], last_sem, (ny if ab else nx) + 1 - c).start()

    def s1(k, jo):
        with jax.named_scope("s1"):
            take(c1_part(c1r, k, jo), c1_sem.at[c1_slot(k, jo)])
        for ab in range(2):
            rows = pl.ds(jo * 256 + ab * B, B)
            p1s[k, jo, ab] = (outs[rows] + c1r[k, 0, rows].astype(F32)).astype(BF)
            across, other = (ny, nx) if ab else (nx, ny)
            plain = rcopy(p1s.at[k, jo, ab], p1r.at[k, jo, ab], sent.at[0], p1_sem.at[k], across)
            if jo:
                skip = jnp.logical_and(k == VIA, last_chip)
            else:
                skip = jnp.logical_and(k == VIA, jnp.logical_and(x + y == 1, (y if ab else x) == 1))

                @pl.when(skip)
                def _():
                    part = p1s.at[k, jo, ab, pl.ds(0, RV)]
                    rcopy(part, extra.at[ab], sent.at[0], extra_sem, other).start()
                    rest = pl.ds(RV, B - RV)
                    src, dst = p1s.at[k, jo, ab, rest], p1r.at[k, jo, ab, rest]
                    rcopy(src, dst, sent.at[0], p1_sem.at[k], across).start()

            pl.when(jnp.logical_not(skip))(plain.start)

    def s1_late():
        @pl.when(last_chip)
        def _():
            with jax.named_scope("late"):
                take(extra, extra_sem)
            for ab in range(2):
                rows = pl.ds(256 + ab * B, RV)
                total = outs[rows] + c1r[VIA, 0, rows].astype(F32) + extra[ab].astype(F32)
                p1s[VIA, 1, ab, 0:RV] = total.astype(BF)
                rcopy(
                    p1s.at[VIA, 1, ab], p1r.at[VIA, 1, ab], sent.at[0], p1_sem.at[VIA], ny if ab else nx
                ).start()

    def s2(k):
        with jax.named_scope("s2"):
            take(c1r.at[k, 1], c1_sem.at[c1_slot(k, 2)])
        alone = jnp.logical_and(k == VIA, first_chip)

        def total(jo, ab):
            rows = pl.ds(jo * 256 + ab * B, B)
            return keep[k, rows] + c1r[k, 1, rows].astype(F32)

        def send(ab):
            rcopy(p2s.at[k, ab], p2r.at[k, ab], sent.at[0], p2_sem.at[k], nx if ab else ny).start()

        @pl.when(alone)
        def _():
            take(dcat.at[0 : 2 * (2 * B - RV) * T // 1024, 0:1024], p1_sem.at[k])
            for ab in range(2):
                mine = total(0, ab)
                p2s[k, ab, 0:RV] = mine[0:RV].astype(BF)
                p2s[k, ab, RV:B] = (mine[RV:B] + p1r[k, 0, ab, RV:B].astype(F32)).astype(BF)
                send(ab)

        @pl.when(jnp.logical_not(alone))
        def _():
            with jax.named_scope("s2"):
                take(p1r.at[k], p1_sem.at[k])
            for ab in range(2):
                p2s[k, ab] = (total(0, ab) + p1r[k, 0, ab].astype(F32)).astype(BF)
                send(ab)

        for ab in range(2):
            keep[k, pl.ds(256 + ab * B, B)] = total(1, ab) + p1r[k, 1, ab].astype(F32)

    @jax.named_scope("s3")
    def s3(k):
        take(p2r.at[k], p2_sem.at[k])
        for ab in range(2):
            done = (keep[k, pl.ds(256 + ab * B, B)] + p2r[k, ab].astype(F32)).astype(BF)
            piece(dx, k, ab, x, y, c)[...] = done.T
            g_send(k, ab, 0)
            g_send(k, ab, 1)
            cf_send(k, ab, 0)

    @jax.named_scope("s4")
    def s4(k):
        take(p1r.at[k], p1_sem.at[k])
        for ab in range(2):

            @pl.when(k < NC - 1)
            def _():
                g_send(k, ab, 2)

            @pl.when(k == NC - 1)
            def _():
                g_send_last(ab)

            cf_send(k, ab, 1)
            cf_send(k, ab, 2)

    @jax.named_scope("s5")
    def s5(k):
        @pl.when(k < NC - 1)
        def _():
            take(p2r.at[k], p2_sem.at[k])
            for ab in range(2):
                cf_send(k, ab, 3)

        @pl.when(jnp.logical_and(k == NC - 1, c == 1))
        def _():
            take(p1r.at[k], last_sem)
            for ab in range(2):
                cf_send(k, ab, 3)
                cf_send(k, ab, 3, h=0, sem=2)

    def exchange(k, lag, fn):
        @pl.when(jnp.logical_and(k >= lag, k < NC + lag))
        def _():
            fn(k - lag)

    def gates(k, slot):
        cols = pl.ds(pl.multiple_of(k * T, T), T)
        for r in range(5):
            rows = slice(r * B, (r + 1) * B)
            g = guc[slot, 0, :, rows].T.astype(F32)
            u = guc[slot, 1, :, rows].T.astype(F32)
            g2 = g * g
            t = jnp.tanh(g * (C0 + (C0 * C1) * g2))
            cdf = 0.5 + 0.5 * t
            act = g * cdf
            slope = cdf + (act * (1.0 - t)) * (C0 + (3.0 * C0 * C1) * g2)
            hid[rows, cols] = (act * u).astype(BF)
            act_s[rows] = act
            slope_s[rows] = u * slope

    def store_grads(k, r, d):
        cols = pl.ds(pl.multiple_of(k * T, T), T)
        dcat[r, cols] = (d * slope_s[r]).astype(BF)
        dcat[F + r.start : F + r.stop, cols] = (d * act_s[r]).astype(BF)

    def halves(n):
        return [slice(i * n // 2, (i + 1) * n // 2) for i in range(2)]

    def term(k, rows):
        return dot(wcat[rows], dcat[:, pl.ds(pl.multiple_of(k * T, T), T)])

    parts = (slice(0, 512), slice(512, 1280), slice(1280, D))

    def load_first(i):
        d = parts[i]
        pltpu.make_async_copy(wd_hbm.at[:, d], wd.at[:, d], first_sem.at[i]).start()
        pltpu.make_async_copy(dy_hbm.at[0:T, d], dyc.at[0, :, d], first_sem.at[i]).start()

    def grads(k, slot, parts, i):
        with jax.named_scope("grads"):
            if not i:
                gates(k, slot)
            for r in halves(F):
                part = dot(wd[r, parts[i]], dyc[slot, :, parts[i]], ((1,), (1,)))
                total = dh[r] + part if i else part
                if i == len(parts) - 1:
                    store_grads(k, r, total)
                else:
                    dh[r] = total

    load_first(0)
    load_gu(0, 0, first_sem.at[0])
    pl.delay(250)
    load_first(1)
    pl.delay(250)
    load_first(2)
    pl.delay(250)
    load_w(0)
    for i, d in enumerate(parts):
        with jax.named_scope("load"):
            n = (T + F) * (d.stop - d.start) + (0 if i else 2 * T * F)
            take(dcat.at[0 : n // 1024, 0:1024], first_sem.at[i])
        if not i:
            load_w(1)
            load_chunk(1, 1)
        grads(0, 0, parts, i)
    load_w(2)
    load_w(3)
    with jax.named_scope("bar"):
        pl.semaphore_wait(barrier, 5)

    def first_use(k, g):
        @pl.when(k == 0)
        def _():
            take(wcat.at[g * 512 : 2048 if g == 2 else (g + 1) * 512], w_sem.at[g])

    def keep_partner(k):
        first_use(k, 2)
        with jax.named_scope("keeps"):
            for r in halves(512):
                c1s[k, 1, r] = term(k, slice(1024 + r.start, 1024 + r.stop)).astype(BF)
        c1_send(k, 2)

    def keep_own(k):
        with jax.named_scope("keeps"):
            for r in halves(512):
                keep[k, r] = term(k, slice(1536 + r.start, 1536 + r.stop))

    def phase1(k, _):
        first_use(k, 0)
        for ab in range(2):
            with jax.named_scope("termP"):
                for i in range(2):
                    r = slice(ab * 256 + i * 128, ab * 256 + (i + 1) * 128)
                    c1s[k, 0, r] = term(k, r).astype(BF)
            c1_send(k, ab)
        first_use(k, 1)
        with jax.named_scope("out"):
            for r in halves(512):
                outs[r] = term(k, slice(512 + r.start, 512 + r.stop))
        s1(k, 0)

        @pl.when(k >= L1)
        def _():
            keep_partner(k - L1)

        nxt = k + 1
        slot = lax.rem(nxt, 2)

        @pl.when(k < NC - 1)
        def _():
            take(dcat.at[0 : (T * D + 2 * T * F) // D], in_sem.at[slot])
            grads(nxt, slot, (slice(0, D),), 0)

            @pl.when(nxt < NC - 1)
            def _():
                load_chunk(nxt + 1, 1 - slot)

            @pl.when(jnp.logical_and(k >= 2, k < 4))
            def _():
                load_panel(k - 2, k - 2)

        s1(k, 1)

        @pl.when(k >= L1)
        def _():
            keep_own(k - L1)

        exchange(k, L2, s2)
        exchange(k, L3, s3)
        exchange(k, L4, s4)
        exchange(k, L5, s5)
        return 0

    lax.fori_loop(0, NC, phase1, 0)

    def last_keeps(k, _):
        keep_partner(k)
        keep_own(k)
        return 0

    lax.fori_loop(NC - L1, NC, last_keeps, 0)

    def phase2(m, _):
        slot = lax.rem(m, 2)
        k = NC + m
        at = pl.ds(pl.multiple_of(m * T, T), T)
        take(pan.at[slot], pan_sem.at[slot])
        with jax.named_scope("dwg"):
            for r in halves(F):
                dwg[at, r] = dot(dcat[r], pan[slot, 0]).astype(BF).T
        pl.when(m == 0)(s1_late)
        exchange(k, L2, s2)
        with jax.named_scope("dwu"):
            for r in halves(F):
                dwu[at, r] = dot(dcat[F + r.start : F + r.stop], pan[slot, 0]).astype(BF).T
        exchange(k, L3, s3)
        exchange(k, L4, s4)
        with jax.named_scope("dwd"):
            for r in halves(F):
                dwd[r, at] = dot(hid[r], pan[slot, 1]).astype(BF)

        @pl.when(m < NC - 2)
        def _():
            load_panel(m + 2, slot)

        exchange(k, L5, s5)
        return 0

    lax.fori_loop(0, NC, phase2, 0)

    def phase3(k, _):
        exchange(k, L4, s4)
        exchange(k, L5, s5)
        return 0

    lax.fori_loop(2 * NC, NC + L5, phase3, 0)
    with jax.named_scope("fin"):
        take(dx.at[0:1536], sent.at[0])

        @pl.when(c == 0)
        def _():
            take(dx.at[0:2016], sent.at[1])
            take(dx.at[0:1056], cf_sem)

        @pl.when(c == 1)
        def _():
            take(dx, sent.at[1])
            take(dx.at[0:32], sent.at[2])
            take(dx.at[0:992], cf_sem)


def write_out(dx, dwg, dwu, dwd, dx_o, dwg_o, dwu_o, dwd_o, sem):
    copies = []
    for src, dst, parts in ((dx, dx_o, 4), (dwg, dwg_o, 2), (dwu, dwu_o, 2), (dwd, dwd_o, 2)):
        n = src.shape[0] // parts
        for i in range(parts):
            rows = pl.ds(i * n, n)
            copies.append(pltpu.make_async_copy(src.at[rows], dst.at[rows], sem.at[len(copies)]))
    for cp in copies:
        cp.start()
    for cp in copies:
        cp.wait()


def solution(mesh):
    def step(x, dy, gate, up, w_gate, w_up, w_down):
        hbm = pl.BlockSpec(memory_space=pltpu.HBM)
        vmem = pl.BlockSpec(memory_space=pltpu.VMEM)
        shapes = ((D, D), (D, F), (D, F), (F, D))
        dma = pltpu.SemaphoreType.DMA
        args = [pltpu.with_memory_space_constraint(a, pltpu.HBM) for a in (x, dy, gate, up, w_gate, w_up, w_down)]
        results = pl.pallas_call(
            kernel,
            out_shape=tuple(pltpu.VMEM(s, BF) for s in shapes),
            in_specs=[hbm] * 7,
            out_specs=(vmem,) * 4,
            scratch_shapes=[
                pltpu.VMEM((D, 2 * F), BF),
                pltpu.VMEM((F, D), BF),
                pltpu.VMEM((2 * F, D), BF),
                pltpu.VMEM((F, D), BF),
                pltpu.VMEM((2, T, D), BF),
                pltpu.VMEM((2, 2, T, F), BF),
                pltpu.VMEM((2, 2, D, T), BF),
                pltpu.VMEM((F, T), F32),
                pltpu.VMEM((F, T), F32),
                pltpu.VMEM((F, T), F32),
                pltpu.VMEM((NC, 512, T), F32),
                pltpu.VMEM((512, T), F32),
                pltpu.VMEM((NC, 2, 512, T), BF),
                pltpu.VMEM((NC, 2, 512, T), BF),
                pltpu.VMEM((NC, 2, 2, B, T), BF),
                pltpu.VMEM((NC, 2, 2, B, T), BF),
                pltpu.VMEM((NC, 2, 128, T), BF),
                pltpu.VMEM((NC, 2, 128, T), BF),
                pltpu.VMEM((2, RV, T), BF),
                dma((2,)),
                dma((3,)),
                dma((3,)),
                dma((2,)),
                dma((8,)),
                dma((NC,)),
                dma((NC,)),
                dma,
                dma((3,)),
                dma,
                dma,
            ],
            compiler_params=pltpu.CompilerParams(
                collective_id=0, has_side_effects=True, vmem_limit_bytes=48 * 2**20
            ),
        )(*args)
        return pl.pallas_call(
            write_out,
            out_shape=tuple(jax.ShapeDtypeStruct(s, BF) for s in shapes),
            in_specs=[vmem] * 4,
            out_specs=(hbm,) * 4,
            scratch_shapes=[dma((10,))],
            compiler_params=pltpu.CompilerParams(vmem_limit_bytes=2**20),
        )(*results)

    tokens, columns, rows = P("dp", None), P(None, "tp"), P("tp", None)
    return jax.shard_map(
        step,
        mesh=mesh,
        in_specs=(tokens, tokens, P("dp", "tp"), P("dp", "tp"), columns, columns, rows),
        out_specs=(tokens, P("dp", "tp"), P("dp", "tp"), P(("dp", "tp"), None)),
        check_vma=False,
    )
```

```python
import functools

import jax
import jax.numpy as jnp
from jax import lax
from jax.experimental import pallas as pl
from jax.experimental.pallas import tpu as pltpu
from jax.sharding import PartitionSpec as P

MESH = pl.DeviceIdType.MESH
BF = jnp.bfloat16
F32 = jnp.float32
T = 256
NC = 8
D = 2048
F = 640
B = 128
L1, L2, L3, L4, L5 = 2, 2, 5, 9, 12
VIA = NC - 1
RV = 112
C0 = 0.7978845608028654
C1 = 0.044715


def dot(a, b, dims=((1,), (0,))):
    return lax.dot_general(a, b, (dims, ((), ())), preferred_element_type=F32)


def kernel(
    x_hbm, dy_hbm, gate_hbm, up_hbm, wg_hbm, wu_hbm, wd_hbm,
    dx, dwg, dwu, dwd,
    wcat, wd, dcat, hid, dyc, guc, pan, dh, act_s, slope_s, keep, outs,
    c1s, c1r, p1s, p1r, p2s, p2r, extra,
    in_sem, first_sem, w_sem, pan_sem,
    c1_sem, p1_sem, p2_sem, cf_sem, sent, extra_sem, last_sem,
):
    me = lax.axis_index("tp")
    c = lax.rem(me, 2)
    y = lax.rem(me // 2, 2)
    x = me // 4
    nx, ny, nc = me + 4 - 8 * x, me + 2 - 4 * y, me + 1 - 2 * c
    first_chip, last_chip = x + y == 0, x + y == 2

    barrier = pltpu.get_barrier_semaphore()
    for to in (nx, ny, nc, nx + 1 - 2 * c, ny + 1 - 2 * c):
        pl.semaphore_signal(barrier, inc=1, device_id={"tp": to}, device_id_type=MESH)

    def rcopy(src, dst, ss, rs, to):
        return pltpu.make_async_remote_copy(
            src_ref=src, dst_ref=dst, send_sem=ss, recv_sem=rs, device_id={"tp": to}, device_id_type=MESH
        )

    def take(ref, sem):
        pltpu.make_async_copy(ref, ref, sem).wait()

    def load_gu(k, s, sem):
        rows = pl.ds(pl.multiple_of(k * T, T), T)
        pltpu.make_async_copy(gate_hbm.at[rows], guc.at[s, 0], sem).start()
        pltpu.make_async_copy(up_hbm.at[rows], guc.at[s, 1], sem).start()

    def load_chunk(k, s):
        rows = pl.ds(pl.multiple_of(k * T, T), T)
        pltpu.make_async_copy(dy_hbm.at[rows], dyc.at[s], in_sem.at[s]).start()
        load_gu(k, s, in_sem.at[s])

    def load_panel(m, s):
        cols = pl.ds(pl.multiple_of(m * T, T), T)
        pltpu.make_async_copy(x_hbm.at[:, cols], pan.at[s, 0], pan_sem.at[s]).start()
        pltpu.make_async_copy(dy_hbm.at[:, cols], pan.at[s, 1], pan_sem.at[s]).start()

    def load_w(g):
        own, kept = g % 2, g // 2
        h = c if own else 1 - c
        for ab in range(2):
            first, second = (x, y) if ab == 0 else (y, x)
            i = first if kept else 1 - first
            for jo in range(2):
                j = second if jo else 1 - second
                src = pl.ds(pl.multiple_of(h * 1024 + ab * 512 + i * 256 + j * 128, B), B)
                dst = pl.ds((g * 4 + jo * 2 + ab) * B, B)
                pltpu.make_async_copy(wg_hbm.at[src], wcat.at[dst, 0:F], w_sem.at[min(g, 2)]).start()
                pltpu.make_async_copy(wu_hbm.at[src], wcat.at[dst, F : 2 * F], w_sem.at[min(g, 2)]).start()

    def piece(ref, k, ab, cx, cy, h):
        col = h * 1024 + (cx * 256 + cy * 128 if ab == 0 else 512 + cy * 256 + cx * 128)
        return ref.at[pl.ds(pl.multiple_of(k * T, T), T), pl.ds(pl.multiple_of(col, B), B)]

    def c1_part(ref, k, part):
        return ref.at[k, 1] if part == 2 else ref.at[k, 0, pl.ds(part * 256, 256)]

    def c1_slot(k, part):
        return 4 + lax.rem(k, 4) if part == 2 else 2 * part + lax.rem(k, 2)

    def c1_send(k, part):
        rcopy(c1_part(c1s, k, part), c1_part(c1r, k, part), sent.at[1], c1_sem.at[c1_slot(k, part)], nc).start()

    def g_send(k, ab, kind):
        far, near = (ny, nx) if ab else (nx, ny)
        if kind == 2:
            ref = piece(dx, k, ab, x, 1 - y, c) if ab == 0 else piece(dx, k, ab, 1 - x, y, c)
        else:
            ref = piece(dx, k, ab, x, y, c)
        rcopy(ref, ref, sent.at[0], (p2_sem if kind == 2 else p1_sem).at[k], near if kind == 0 else far).start()

    def cf_send(k, ab, which, h=c, sem=1):
        cx, cy = ((x, y), (x, 1 - y), (1 - x, y), (1 - x, 1 - y))[which]
        ref = piece(dx, k, ab, cx, cy, h)
        rcopy(ref, ref, sent.at[sem], cf_sem, nc).start()

    def g_send_last(ab):
        cx, cy = (x, 1 - y) if ab == 0 else (1 - x, y)
        ref = piece(dx, NC - 1, ab, cx, cy, c)
        rcopy(ref, ref, sent.at[0], last_sem.at[ab], (ny if ab else nx) + 1 - c).start()

    def s1(k, jo):
        with jax.named_scope("s1"):
            take(c1_part(c1r, k, jo), c1_sem.at[c1_slot(k, jo)])
        for ab in range(2):
            rows = pl.ds(jo * 256 + ab * B, B)
            p1s[k, jo, ab] = (outs[rows] + c1r[k, 0, rows].astype(F32)).astype(BF)
            across, other = (ny, nx) if ab else (nx, ny)
            plain = rcopy(p1s.at[k, jo, ab], p1r.at[k, jo, ab], sent.at[0], p1_sem.at[k], across)
            if jo:
                skip = jnp.logical_and(k == VIA, last_chip)
            else:
                skip = jnp.logical_and(k == VIA, jnp.logical_and(x + y == 1, (y if ab else x) == 1))

                @pl.when(skip)
                def _():
                    part = p1s.at[k, jo, ab, pl.ds(0, RV)]
                    rcopy(part, extra.at[ab], sent.at[0], extra_sem, other).start()
                    rest = pl.ds(RV, B - RV)
                    src, dst = p1s.at[k, jo, ab, rest], p1r.at[k, jo, ab, rest]
                    rcopy(src, dst, sent.at[0], p1_sem.at[k], across).start()

            pl.when(jnp.logical_not(skip))(plain.start)

    def s1_late():
        @pl.when(last_chip)
        def _():
            with jax.named_scope("late"):
                take(extra, extra_sem)
            for ab in range(2):
                rows = pl.ds(256 + ab * B, RV)
                total = outs[rows] + c1r[VIA, 0, rows].astype(F32) + extra[ab].astype(F32)
                p1s[VIA, 1, ab, 0:RV] = total.astype(BF)
                rcopy(
                    p1s.at[VIA, 1, ab], p1r.at[VIA, 1, ab], sent.at[0], p1_sem.at[VIA], ny if ab else nx
                ).start()

    def s2(k):
        with jax.named_scope("s2"):
            take(c1r.at[k, 1], c1_sem.at[c1_slot(k, 2)])
        alone = jnp.logical_and(k == VIA, first_chip)

        def total(jo, ab):
            rows = pl.ds(jo * 256 + ab * B, B)
            return keep[k, rows] + c1r[k, 1, rows].astype(F32)

        def send(ab):
            rcopy(p2s.at[k, ab], p2r.at[k, ab], sent.at[0], p2_sem.at[k], nx if ab else ny).start()

        @pl.when(alone)
        def _():
            take(dcat.at[0 : 2 * (2 * B - RV) * T // 1024, 0:1024], p1_sem.at[k])
            for ab in range(2):
                mine = total(0, ab)
                p2s[k, ab, 0:RV] = mine[0:RV].astype(BF)
                p2s[k, ab, RV:B] = (mine[RV:B] + p1r[k, 0, ab, RV:B].astype(F32)).astype(BF)
                send(ab)

        @pl.when(jnp.logical_not(alone))
        def _():
            with jax.named_scope("s2"):
                take(p1r.at[k], p1_sem.at[k])
            for ab in range(2):
                p2s[k, ab] = (total(0, ab) + p1r[k, 0, ab].astype(F32)).astype(BF)
                send(ab)

        for ab in range(2):
            keep[k, pl.ds(256 + ab * B, B)] = total(1, ab) + p1r[k, 1, ab].astype(F32)

    @jax.named_scope("s3")
    def s3(k):
        take(p2r.at[k], p2_sem.at[k])
        for ab in range(2):
            done = (keep[k, pl.ds(256 + ab * B, B)] + p2r[k, ab].astype(F32)).astype(BF)
            piece(dx, k, ab, x, y, c)[...] = done.T
            g_send(k, ab, 0)
            g_send(k, ab, 1)
            cf_send(k, ab, 0)

    @jax.named_scope("s4")
    def s4(k):
        take(p1r.at[k], p1_sem.at[k])
        for ab in range(2):

            @pl.when(k < NC - 1)
            def _():
                g_send(k, ab, 2)

            @pl.when(k == NC - 1)
            def _():
                g_send_last(ab)

            cf_send(k, ab, 1)
            cf_send(k, ab, 2)

    @jax.named_scope("s5")
    def s5(k):
        @pl.when(k < NC - 1)
        def _():
            take(p2r.at[k], p2_sem.at[k])
            for ab in range(2):
                cf_send(k, ab, 3)

        @pl.when(jnp.logical_and(k == NC - 1, c == 1))
        def _():
            for ab in range(2):
                take(p2r.at[k], last_sem.at[ab])
                cf_send(k, ab, 3)
                cf_send(k, ab, 3, h=0, sem=2)

    def exchange(k, lag, fn):
        @pl.when(jnp.logical_and(k >= lag, k < NC + lag))
        def _():
            fn(k - lag)

    def gates(k, slot):
        cols = pl.ds(pl.multiple_of(k * T, T), T)
        for r in range(5):
            rows = slice(r * B, (r + 1) * B)
            g = guc[slot, 0, :, rows].T.astype(F32)
            u = guc[slot, 1, :, rows].T.astype(F32)
            g2 = g * g
            t = jnp.tanh(g * (C0 + (C0 * C1) * g2))
            cdf = 0.5 + 0.5 * t
            act = g * cdf
            slope = cdf + (act * (1.0 - t)) * (C0 + (3.0 * C0 * C1) * g2)
            hid[rows, cols] = (act * u).astype(BF)
            act_s[rows] = act
            slope_s[rows] = u * slope

    def store_grads(k, r, d):
        cols = pl.ds(pl.multiple_of(k * T, T), T)
        dcat[r, cols] = (d * slope_s[r]).astype(BF)
        dcat[F + r.start : F + r.stop, cols] = (d * act_s[r]).astype(BF)

    def halves(n):
        return [slice(i * n // 2, (i + 1) * n // 2) for i in range(2)]

    def term(k, rows):
        return dot(wcat[rows], dcat[:, pl.ds(pl.multiple_of(k * T, T), T)])

    parts = (slice(0, 512), slice(512, 1280), slice(1280, D))

    def load_first(i):
        d = parts[i]
        pltpu.make_async_copy(wd_hbm.at[:, d], wd.at[:, d], first_sem.at[i]).start()
        pltpu.make_async_copy(dy_hbm.at[0:T, d], dyc.at[0, :, d], first_sem.at[i]).start()

    def grads(k, slot, parts, i):
        with jax.named_scope("grads"):
            if not i:
                gates(k, slot)
            for r in halves(F):
                part = dot(wd[r, parts[i]], dyc[slot, :, parts[i]], ((1,), (1,)))
                total = dh[r] + part if i else part
                if i == len(parts) - 1:
                    store_grads(k, r, total)
                else:
                    dh[r] = total

    load_first(0)
    load_gu(0, 0, first_sem.at[0])
    pl.delay(250)
    load_first(1)
    pl.delay(250)
    load_first(2)
    pl.delay(250)
    load_w(0)
    for i, d in enumerate(parts):
        with jax.named_scope("load"):
            n = (T + F) * (d.stop - d.start) + (0 if i else 2 * T * F)
            take(dcat.at[0 : n // 1024, 0:1024], first_sem.at[i])
        if not i:
            load_w(1)
            load_chunk(1, 1)
        grads(0, 0, parts, i)
    load_w(2)
    load_w(3)
    with jax.named_scope("bar"):
        pl.semaphore_wait(barrier, 5)

    def first_use(k, g):
        @pl.when(k == 0)
        def _():
            take(wcat.at[g * 512 : 2048 if g == 2 else (g + 1) * 512], w_sem.at[g])

    def keep_partner(k):
        first_use(k, 2)
        with jax.named_scope("keeps"):
            for r in halves(512):
                c1s[k, 1, r] = term(k, slice(1024 + r.start, 1024 + r.stop)).astype(BF)
        c1_send(k, 2)

    def keep_own(k):
        with jax.named_scope("keeps"):
            for r in halves(512):
                keep[k, r] = term(k, slice(1536 + r.start, 1536 + r.stop))

    def phase1(k, _):
        first_use(k, 0)
        for ab in range(2):
            with jax.named_scope("termP"):
                for i in range(2):
                    r = slice(ab * 256 + i * 128, ab * 256 + (i + 1) * 128)
                    c1s[k, 0, r] = term(k, r).astype(BF)
            c1_send(k, ab)
        first_use(k, 1)
        with jax.named_scope("out"):
            for r in halves(512):
                outs[r] = term(k, slice(512 + r.start, 512 + r.stop))
        s1(k, 0)

        @pl.when(k >= L1)
        def _():
            keep_partner(k - L1)

        nxt = k + 1
        slot = lax.rem(nxt, 2)

        @pl.when(k < NC - 1)
        def _():
            take(dcat.at[0 : (T * D + 2 * T * F) // D], in_sem.at[slot])
            grads(nxt, slot, (slice(0, D),), 0)

            @pl.when(nxt < NC - 1)
            def _():
                load_chunk(nxt + 1, 1 - slot)

            @pl.when(jnp.logical_and(k >= 2, k < 4))
            def _():
                load_panel(k - 2, k - 2)

        s1(k, 1)

        @pl.when(k >= L1)
        def _():
            keep_own(k - L1)

        exchange(k, L2, s2)
        exchange(k, L3, s3)
        exchange(k, L4, s4)
        exchange(k, L5, s5)
        return 0

    lax.fori_loop(0, NC, phase1, 0)

    def last_keeps(k, _):
        keep_partner(k)
        keep_own(k)
        return 0

    lax.fori_loop(NC - L1, NC, last_keeps, 0)

    def phase2(m, _):
        slot = lax.rem(m, 2)
        k = NC + m
        at = pl.ds(pl.multiple_of(m * T, T), T)
        take(pan.at[slot], pan_sem.at[slot])
        with jax.named_scope("dwg"):
            for r in halves(F):
                dwg[at, r] = dot(dcat[r], pan[slot, 0]).astype(BF).T
        pl.when(m == 0)(s1_late)
        exchange(k, L2, s2)
        with jax.named_scope("dwu"):
            for r in halves(F):
                dwu[at, r] = dot(dcat[F + r.start : F + r.stop], pan[slot, 0]).astype(BF).T
        exchange(k, L3, s3)
        exchange(k, L4, s4)
        with jax.named_scope("dwd"):
            for r in halves(F):
                dwd[r, at] = dot(hid[r], pan[slot, 1]).astype(BF)

        @pl.when(m < NC - 2)
        def _():
            load_panel(m + 2, slot)

        exchange(k, L5, s5)
        return 0

    lax.fori_loop(0, NC, phase2, 0)

    def phase3(k, _):
        exchange(k, L4, s4)
        exchange(k, L5, s5)
        return 0

    lax.fori_loop(2 * NC, NC + L5, phase3, 0)
    with jax.named_scope("fin"):
        take(dx.at[0:1536], sent.at[0])

        @pl.when(c == 0)
        def _():
            take(dx.at[0:2016], sent.at[1])
            take(dx.at[0:1056], cf_sem)

        @pl.when(c == 1)
        def _():
            take(dx, sent.at[1])
            take(dx.at[0:32], sent.at[2])
            take(dx.at[0:992], cf_sem)


def write_out(dx, dwg, dwu, dwd, dx_o, dwg_o, dwu_o, dwd_o, sem):
    copies = []
    for src, dst, parts in ((dx, dx_o, 4), (dwg, dwg_o, 2), (dwu, dwu_o, 2), (dwd, dwd_o, 2)):
        n = src.shape[0] // parts
        for i in range(parts):
            rows = pl.ds(i * n, n)
            copies.append(pltpu.make_async_copy(src.at[rows], dst.at[rows], sem.at[len(copies)]))
    for cp in copies:
        cp.start()
    for cp in copies:
        cp.wait()


def solution(mesh):
    def step(x, dy, gate, up, w_gate, w_up, w_down):
        hbm = pl.BlockSpec(memory_space=pltpu.HBM)
        vmem = pl.BlockSpec(memory_space=pltpu.VMEM)
        shapes = ((D, D), (D, F), (D, F), (F, D))
        dma = pltpu.SemaphoreType.DMA
        args = [pltpu.with_memory_space_constraint(a, pltpu.HBM) for a in (x, dy, gate, up, w_gate, w_up, w_down)]
        results = pl.pallas_call(
            kernel,
            out_shape=tuple(pltpu.VMEM(s, BF) for s in shapes),
            in_specs=[hbm] * 7,
            out_specs=(vmem,) * 4,
            scratch_shapes=[
                pltpu.VMEM((D, 2 * F), BF),
                pltpu.VMEM((F, D), BF),
                pltpu.VMEM((2 * F, D), BF),
                pltpu.VMEM((F, D), BF),
                pltpu.VMEM((2, T, D), BF),
                pltpu.VMEM((2, 2, T, F), BF),
                pltpu.VMEM((2, 2, D, T), BF),
                pltpu.VMEM((F, T), F32),
                pltpu.VMEM((F, T), F32),
                pltpu.VMEM((F, T), F32),
                pltpu.VMEM((NC, 512, T), F32),
                pltpu.VMEM((512, T), F32),
                pltpu.VMEM((NC, 2, 512, T), BF),
                pltpu.VMEM((NC, 2, 512, T), BF),
                pltpu.VMEM((NC, 2, 2, B, T), BF),
                pltpu.VMEM((NC, 2, 2, B, T), BF),
                pltpu.VMEM((NC, 2, 128, T), BF),
                pltpu.VMEM((NC, 2, 128, T), BF),
                pltpu.VMEM((2, RV, T), BF),
                dma((2,)),
                dma((3,)),
                dma((3,)),
                dma((2,)),
                dma((8,)),
                dma((NC,)),
                dma((NC,)),
                dma,
                dma((3,)),
                dma,
                dma((2,)),
            ],
            compiler_params=pltpu.CompilerParams(
                collective_id=0, has_side_effects=True, vmem_limit_bytes=48 * 2**20
            ),
        )(*args)
        return pl.pallas_call(
            write_out,
            out_shape=tuple(jax.ShapeDtypeStruct(s, BF) for s in shapes),
            in_specs=[vmem] * 4,
            out_specs=(hbm,) * 4,
            scratch_shapes=[dma((10,))],
            compiler_params=pltpu.CompilerParams(vmem_limit_bytes=2**20),
        )(*results)

    tokens, columns, rows = P("dp", None), P(None, "tp"), P("tp", None)
    return jax.shard_map(
        step,
        mesh=mesh,
        in_specs=(tokens, tokens, P("dp", "tp"), P("dp", "tp"), columns, columns, rows),
        out_specs=(tokens, P("dp", "tp"), P("dp", "tp"), P(("dp", "tp"), None)),
        check_vma=False,
    )
```

```python
import functools

import jax
import jax.numpy as jnp
from jax import lax
from jax.experimental import pallas as pl
from jax.experimental.pallas import tpu as pltpu
from jax.sharding import PartitionSpec as P

MESH = pl.DeviceIdType.MESH
BF = jnp.bfloat16
F32 = jnp.float32
T = 256
NC = 8
D = 2048
F = 640
B = 128
L1, L2, L3, L4, L5 = 2, 2, 5, 9, 12
VIA = NC - 1
RV = 112
C0 = 0.7978845608028654
C1 = 0.044715


def dot(a, b, dims=((1,), (0,))):
    return lax.dot_general(a, b, (dims, ((), ())), preferred_element_type=F32)


def kernel(
    x_hbm, dy_hbm, gate_hbm, up_hbm, wg_hbm, wu_hbm, wd_hbm,
    dx, dwg, dwu, dwd,
    wcat, wd, dcat, hid, dyc, guc, pan, dh, act_s, slope_s, keep, outs,
    c1s, c1r, p1s, p1r, p2s, p2r, extra,
    in_sem, first_sem, w_sem, pan_sem,
    c1_sem, p1_sem, p2_sem, cf_sem, sent, extra_sem, last_sem,
):
    me = lax.axis_index("tp")
    c = lax.rem(me, 2)
    y = lax.rem(me // 2, 2)
    x = me // 4
    nx, ny, nc = me + 4 - 8 * x, me + 2 - 4 * y, me + 1 - 2 * c
    first_chip, last_chip = x + y == 0, x + y == 2

    def rcopy(src, dst, ss, rs, to):
        return pltpu.make_async_remote_copy(
            src_ref=src, dst_ref=dst, send_sem=ss, recv_sem=rs, device_id={"tp": to}, device_id_type=MESH
        )

    def take(ref, sem):
        pltpu.make_async_copy(ref, ref, sem).wait()

    def load_gu(k, s, sem):
        rows = pl.ds(pl.multiple_of(k * T, T), T)
        pltpu.make_async_copy(gate_hbm.at[rows], guc.at[s, 0], sem).start()
        pltpu.make_async_copy(up_hbm.at[rows], guc.at[s, 1], sem).start()

    def load_chunk(k, s):
        rows = pl.ds(pl.multiple_of(k * T, T), T)
        pltpu.make_async_copy(dy_hbm.at[rows], dyc.at[s], in_sem.at[s]).start()
        load_gu(k, s, in_sem.at[s])

    def load_panel(m, s):
        cols = pl.ds(pl.multiple_of(m * T, T), T)
        pltpu.make_async_copy(x_hbm.at[:, cols], pan.at[s, 0], pan_sem.at[s]).start()
        pltpu.make_async_copy(dy_hbm.at[:, cols], pan.at[s, 1], pan_sem.at[s]).start()

    def load_w(g):
        own, kept = g % 2, g // 2
        h = c if own else 1 - c
        for ab in range(2):
            first, second = (x, y) if ab == 0 else (y, x)
            i = first if kept else 1 - first
            for jo in range(2):
                j = second if jo else 1 - second
                src = pl.ds(pl.multiple_of(h * 1024 + ab * 512 + i * 256 + j * 128, B), B)
                dst = pl.ds((g * 4 + jo * 2 + ab) * B, B)
                pltpu.make_async_copy(wg_hbm.at[src], wcat.at[dst, 0:F], w_sem.at[min(g, 2)]).start()
                pltpu.make_async_copy(wu_hbm.at[src], wcat.at[dst, F : 2 * F], w_sem.at[min(g, 2)]).start()

    def piece(ref, k, ab, cx, cy, h):
        col = h * 1024 + (cx * 256 + cy * 128 if ab == 0 else 512 + cy * 256 + cx * 128)
        return ref.at[pl.ds(pl.multiple_of(k * T, T), T), pl.ds(pl.multiple_of(col, B), B)]

    def c1_part(ref, k, part):
        return ref.at[k, 1] if part == 2 else ref.at[k, 0, pl.ds(part * 256, 256)]

    def c1_slot(k, part):
        return 4 + lax.rem(k, 4) if part == 2 else 2 * part + lax.rem(k, 2)

    def c1_send(k, part):
        rcopy(c1_part(c1s, k, part), c1_part(c1r, k, part), sent.at[1], c1_sem.at[c1_slot(k, part)], nc).start()

    def g_send(k, ab, kind):
        far, near = (ny, nx) if ab else (nx, ny)
        if kind == 2:
            ref = piece(dx, k, ab, x, 1 - y, c) if ab == 0 else piece(dx, k, ab, 1 - x, y, c)
        else:
            ref = piece(dx, k, ab, x, y, c)
        rcopy(ref, ref, sent.at[0], (p2_sem if kind == 2 else p1_sem).at[k], near if kind == 0 else far).start()

    def cf_send(k, ab, which, h=c, sem=1):
        cx, cy = ((x, y), (x, 1 - y), (1 - x, y), (1 - x, 1 - y))[which]
        ref = piece(dx, k, ab, cx, cy, h)
        rcopy(ref, ref, sent.at[sem], cf_sem, nc).start()

    def g_send_last(ab):
        cx, cy = (x, 1 - y) if ab == 0 else (1 - x, y)
        ref = piece(dx, NC - 1, ab, cx, cy, c)
        rcopy(ref, ref, sent.at[0], last_sem.at[ab], (ny if ab else nx) + 1 - c).start()

    def s1(k, jo):
        with jax.named_scope("s1"):
            take(c1_part(c1r, k, jo), c1_sem.at[c1_slot(k, jo)])
        for ab in range(2):
            rows = pl.ds(jo * 256 + ab * B, B)
            p1s[k, jo, ab] = (outs[rows] + c1r[k, 0, rows].astype(F32)).astype(BF)
            across, other = (ny, nx) if ab else (nx, ny)
            plain = rcopy(p1s.at[k, jo, ab], p1r.at[k, jo, ab], sent.at[0], p1_sem.at[k], across)
            if jo:
                skip = jnp.logical_and(k == VIA, last_chip)
            else:
                skip = jnp.logical_and(k == VIA, jnp.logical_and(x + y == 1, (y if ab else x) == 1))

                @pl.when(skip)
                def _():
                    part = p1s.at[k, jo, ab, pl.ds(0, RV)]
                    rcopy(part, extra.at[ab], sent.at[0], extra_sem, other).start()
                    rest = pl.ds(RV, B - RV)
                    src, dst = p1s.at[k, jo, ab, rest], p1r.at[k, jo, ab, rest]
                    rcopy(src, dst, sent.at[0], p1_sem.at[k], across).start()

            pl.when(jnp.logical_not(skip))(plain.start)

    def s1_late():
        @pl.when(last_chip)
        def _():
            with jax.named_scope("late"):
                take(extra, extra_sem)
            for ab in range(2):
                rows = pl.ds(256 + ab * B, RV)
                total = outs[rows] + c1r[VIA, 0, rows].astype(F32) + extra[ab].astype(F32)
                p1s[VIA, 1, ab, 0:RV] = total.astype(BF)
                rcopy(
                    p1s.at[VIA, 1, ab], p1r.at[VIA, 1, ab], sent.at[0], p1_sem.at[VIA], ny if ab else nx
                ).start()

    def s2(k):
        with jax.named_scope("s2"):
            take(c1r.at[k, 1], c1_sem.at[c1_slot(k, 2)])
        alone = jnp.logical_and(k == VIA, first_chip)

        def total(jo, ab):
            rows = pl.ds(jo * 256 + ab * B, B)
            return keep[k, rows] + c1r[k, 1, rows].astype(F32)

        def send(ab):
            rcopy(p2s.at[k, ab], p2r.at[k, ab], sent.at[0], p2_sem.at[k], nx if ab else ny).start()

        @pl.when(alone)
        def _():
            take(dcat.at[0 : 2 * (2 * B - RV) * T // 1024, 0:1024], p1_sem.at[k])
            for ab in range(2):
                mine = total(0, ab)
                p2s[k, ab, 0:RV] = mine[0:RV].astype(BF)
                p2s[k, ab, RV:B] = (mine[RV:B] + p1r[k, 0, ab, RV:B].astype(F32)).astype(BF)
                send(ab)

        @pl.when(jnp.logical_not(alone))
        def _():
            with jax.named_scope("s2"):
                take(p1r.at[k], p1_sem.at[k])
            for ab in range(2):
                p2s[k, ab] = (total(0, ab) + p1r[k, 0, ab].astype(F32)).astype(BF)
                send(ab)

        for ab in range(2):
            keep[k, pl.ds(256 + ab * B, B)] = total(1, ab) + p1r[k, 1, ab].astype(F32)

    @jax.named_scope("s3")
    def s3(k):
        take(p2r.at[k], p2_sem.at[k])
        for ab in range(2):
            done = (keep[k, pl.ds(256 + ab * B, B)] + p2r[k, ab].astype(F32)).astype(BF)
            piece(dx, k, ab, x, y, c)[...] = done.T
            g_send(k, ab, 0)
            g_send(k, ab, 1)
            cf_send(k, ab, 0)

    @jax.named_scope("s4")
    def s4(k):
        take(p1r.at[k], p1_sem.at[k])
        for ab in range(2):

            @pl.when(k < NC - 1)
            def _():
                g_send(k, ab, 2)

            @pl.when(k == NC - 1)
            def _():
                g_send_last(ab)

            cf_send(k, ab, 1)
            cf_send(k, ab, 2)

    @jax.named_scope("s5")
    def s5(k):
        @pl.when(k < NC - 1)
        def _():
            take(p2r.at[k], p2_sem.at[k])
            for ab in range(2):
                cf_send(k, ab, 3)

        @pl.when(jnp.logical_and(k == NC - 1, c == 1))
        def _():
            for ab in range(2):
                take(p2r.at[k], last_sem.at[ab])
                cf_send(k, ab, 3)
                cf_send(k, ab, 3, h=0, sem=2)

    def exchange(k, lag, fn):
        @pl.when(jnp.logical_and(k >= lag, k < NC + lag))
        def _():
            fn(k - lag)

    def gates(k, slot):
        cols = pl.ds(pl.multiple_of(k * T, T), T)
        for r in range(5):
            rows = slice(r * B, (r + 1) * B)
            g = guc[slot, 0, :, rows].T.astype(F32)
            u = guc[slot, 1, :, rows].T.astype(F32)
            g2 = g * g
            t = jnp.tanh(g * (C0 + (C0 * C1) * g2))
            cdf = 0.5 + 0.5 * t
            act = g * cdf
            slope = cdf + (act * (1.0 - t)) * (C0 + (3.0 * C0 * C1) * g2)
            hid[rows, cols] = (act * u).astype(BF)
            act_s[rows] = act
            slope_s[rows] = u * slope

    def store_grads(k, r, d):
        cols = pl.ds(pl.multiple_of(k * T, T), T)
        dcat[r, cols] = (d * slope_s[r]).astype(BF)
        dcat[F + r.start : F + r.stop, cols] = (d * act_s[r]).astype(BF)

    def halves(n):
        return [slice(i * n // 2, (i + 1) * n // 2) for i in range(2)]

    def term(k, rows):
        return dot(wcat[rows], dcat[:, pl.ds(pl.multiple_of(k * T, T), T)])

    parts = (slice(0, 512), slice(512, 1280), slice(1280, D))

    def load_first(i):
        d = parts[i]
        pltpu.make_async_copy(wd_hbm.at[:, d], wd.at[:, d], first_sem.at[i]).start()
        pltpu.make_async_copy(dy_hbm.at[0:T, d], dyc.at[0, :, d], first_sem.at[i]).start()

    def grads(k, slot, parts, i):
        with jax.named_scope("grads"):
            if not i:
                gates(k, slot)
            for r in halves(F):
                part = dot(wd[r, parts[i]], dyc[slot, :, parts[i]], ((1,), (1,)))
                total = dh[r] + part if i else part
                if i == len(parts) - 1:
                    store_grads(k, r, total)
                else:
                    dh[r] = total

    load_first(0)
    load_gu(0, 0, first_sem.at[0])
    barrier = pltpu.get_barrier_semaphore()
    for to in (nx, ny, nc, nx + 1 - 2 * c, ny + 1 - 2 * c):
        pl.semaphore_signal(barrier, inc=1, device_id={"tp": to}, device_id_type=MESH)
    pl.delay(250)
    load_first(1)
    pl.delay(250)
    load_first(2)
    pl.delay(250)
    load_w(0)
    for i, d in enumerate(parts):
        with jax.named_scope("load"):
            n = (T + F) * (d.stop - d.start) + (0 if i else 2 * T * F)
            take(dcat.at[0 : n // 1024, 0:1024], first_sem.at[i])
        if not i:
            load_w(1)
            load_chunk(1, 1)
        grads(0, 0, parts, i)
    load_w(2)
    load_w(3)
    with jax.named_scope("bar"):
        pl.semaphore_wait(barrier, 5)

    def first_use(k, g):
        @pl.when(k == 0)
        def _():
            take(wcat.at[g * 512 : 2048 if g == 2 else (g + 1) * 512], w_sem.at[g])

    def keep_partner(k):
        first_use(k, 2)
        with jax.named_scope("keeps"):
            for r in halves(512):
                c1s[k, 1, r] = term(k, slice(1024 + r.start, 1024 + r.stop)).astype(BF)
        c1_send(k, 2)

    def keep_own(k):
        with jax.named_scope("keeps"):
            for r in halves(512):
                keep[k, r] = term(k, slice(1536 + r.start, 1536 + r.stop))

    def phase1(k, _):
        first_use(k, 0)
        for ab in range(2):
            with jax.named_scope("termP"):
                for i in range(2):
                    r = slice(ab * 256 + i * 128, ab * 256 + (i + 1) * 128)
                    c1s[k, 0, r] = term(k, r).astype(BF)
            c1_send(k, ab)
        first_use(k, 1)
        with jax.named_scope("out"):
            for r in halves(512):
                outs[r] = term(k, slice(512 + r.start, 512 + r.stop))
        s1(k, 0)

        @pl.when(k >= L1)
        def _():
            keep_partner(k - L1)

        nxt = k + 1
        slot = lax.rem(nxt, 2)

        @pl.when(k < NC - 1)
        def _():
            take(dcat.at[0 : (T * D + 2 * T * F) // D], in_sem.at[slot])
            grads(nxt, slot, (slice(0, D),), 0)

            @pl.when(nxt < NC - 1)
            def _():
                load_chunk(nxt + 1, 1 - slot)

            @pl.when(jnp.logical_and(k >= 2, k < 4))
            def _():
                load_panel(k - 2, k - 2)

        s1(k, 1)

        @pl.when(k >= L1)
        def _():
            keep_own(k - L1)

        exchange(k, L2, s2)
        exchange(k, L3, s3)
        exchange(k, L4, s4)
        exchange(k, L5, s5)
        return 0

    lax.fori_loop(0, NC, phase1, 0)

    def last_keeps(k, _):
        keep_partner(k)
        keep_own(k)
        return 0

    lax.fori_loop(NC - L1, NC, last_keeps, 0)

    def phase2(m, _):
        slot = lax.rem(m, 2)
        k = NC + m
        at = pl.ds(pl.multiple_of(m * T, T), T)
        take(pan.at[slot], pan_sem.at[slot])
        with jax.named_scope("dwg"):
            for r in halves(F):
                dwg[at, r] = dot(dcat[r], pan[slot, 0]).astype(BF).T
        pl.when(m == 0)(s1_late)
        exchange(k, L2, s2)
        with jax.named_scope("dwu"):
            for r in halves(F):
                dwu[at, r] = dot(dcat[F + r.start : F + r.stop], pan[slot, 0]).astype(BF).T
        exchange(k, L3, s3)
        exchange(k, L4, s4)
        with jax.named_scope("dwd"):
            for r in halves(F):
                dwd[r, at] = dot(hid[r], pan[slot, 1]).astype(BF)

        @pl.when(m < NC - 2)
        def _():
            load_panel(m + 2, slot)

        exchange(k, L5, s5)
        return 0

    lax.fori_loop(0, NC, phase2, 0)

    def phase3(k, _):
        exchange(k, L4, s4)
        exchange(k, L5, s5)
        return 0

    lax.fori_loop(2 * NC, NC + L5, phase3, 0)
    with jax.named_scope("fin"):
        take(dx.at[0:1536], sent.at[0])

        @pl.when(c == 0)
        def _():
            take(dx.at[0:2016], sent.at[1])
            take(dx.at[0:1056], cf_sem)

        @pl.when(c == 1)
        def _():
            take(dx, sent.at[1])
            take(dx.at[0:32], sent.at[2])
            take(dx.at[0:992], cf_sem)


def write_out(dx, dwg, dwu, dwd, dx_o, dwg_o, dwu_o, dwd_o, sem):
    pairs = ((dx, dx_o, 4), (dwg, dwg_o, 2), (dwu, dwu_o, 2), (dwd, dwd_o, 2))
    for k, (src, dst, parts) in enumerate(pairs):
        n = src.shape[0] // parts
        for i in range(parts):
            rows = pl.ds(i * n, n)
            pltpu.make_async_copy(src.at[rows], dst.at[rows], sem.at[k]).start()
    for k, (src, dst, _) in enumerate(pairs):
        pltpu.make_async_copy(src, dst, sem.at[k]).wait()


def solution(mesh):
    def step(x, dy, gate, up, w_gate, w_up, w_down):
        hbm = pl.BlockSpec(memory_space=pltpu.HBM)
        vmem = pl.BlockSpec(memory_space=pltpu.VMEM)
        shapes = ((D, D), (D, F), (D, F), (F, D))
        dma = pltpu.SemaphoreType.DMA
        args = [pltpu.with_memory_space_constraint(a, pltpu.HBM) for a in (x, dy, gate, up, w_gate, w_up, w_down)]
        results = pl.pallas_call(
            kernel,
            out_shape=tuple(pltpu.VMEM(s, BF) for s in shapes),
            in_specs=[hbm] * 7,
            out_specs=(vmem,) * 4,
            scratch_shapes=[
                pltpu.VMEM((D, 2 * F), BF),
                pltpu.VMEM((F, D), BF),
                pltpu.VMEM((2 * F, D), BF),
                pltpu.VMEM((F, D), BF),
                pltpu.VMEM((2, T, D), BF),
                pltpu.VMEM((2, 2, T, F), BF),
                pltpu.VMEM((2, 2, D, T), BF),
                pltpu.VMEM((F, T), F32),
                pltpu.VMEM((F, T), F32),
                pltpu.VMEM((F, T), F32),
                pltpu.VMEM((NC, 512, T), F32),
                pltpu.VMEM((512, T), F32),
                pltpu.VMEM((NC, 2, 512, T), BF),
                pltpu.VMEM((NC, 2, 512, T), BF),
                pltpu.VMEM((NC, 2, 2, B, T), BF),
                pltpu.VMEM((NC, 2, 2, B, T), BF),
                pltpu.VMEM((NC, 2, 128, T), BF),
                pltpu.VMEM((NC, 2, 128, T), BF),
                pltpu.VMEM((2, RV, T), BF),
                dma((2,)),
                dma((3,)),
                dma((3,)),
                dma((2,)),
                dma((8,)),
                dma((NC,)),
                dma((NC,)),
                dma,
                dma((3,)),
                dma,
                dma((2,)),
            ],
            compiler_params=pltpu.CompilerParams(
                collective_id=0, has_side_effects=True, vmem_limit_bytes=48 * 2**20
            ),
        )(*args)
        return pl.pallas_call(
            write_out,
            out_shape=tuple(jax.ShapeDtypeStruct(s, BF) for s in shapes),
            in_specs=[vmem] * 4,
            out_specs=(hbm,) * 4,
            scratch_shapes=[dma((4,))],
            compiler_params=pltpu.CompilerParams(vmem_limit_bytes=2**20),
        )(*results)

    tokens, columns, rows = P("dp", None), P(None, "tp"), P("tp", None)
    return jax.shard_map(
        step,
        mesh=mesh,
        in_specs=(tokens, tokens, P("dp", "tp"), P("dp", "tp"), columns, columns, rows),
        out_specs=(tokens, P("dp", "tp"), P("dp", "tp"), P(("dp", "tp"), None)),
        check_vma=False,
    )
```

```python
import functools

import jax
import jax.numpy as jnp
from jax import lax
from jax.experimental import pallas as pl
from jax.experimental.pallas import tpu as pltpu
from jax.sharding import PartitionSpec as P

MESH = pl.DeviceIdType.MESH
BF = jnp.bfloat16
F32 = jnp.float32
T = 256
NC = 8
D = 2048
F = 640
B = 128
L1, L2, L3, L4, L5 = 2, 2, 5, 9, 12
VIA = NC - 1
RV = 112
C0 = 0.7978845608028654
C1 = 0.044715


def dot(a, b, dims=((1,), (0,))):
    return lax.dot_general(a, b, (dims, ((), ())), preferred_element_type=F32)


def kernel(
    x_hbm, dy_hbm, gate_hbm, up_hbm, wg_hbm, wu_hbm, wd_hbm,
    dx, dwg, dwu, dwd,
    wcat, wd, dcat, hid, dyc, guc, pan, dh, act_s, slope_s, keep, outs,
    c1s, c1r, p1s, p1r, p2s, p2r, extra,
    in_sem, first_sem, w_sem,
    c1_sem, p1_sem, p2_sem, cf_sem, sent, extra_sem, last_sem,
):
    me = lax.axis_index("tp")
    c = lax.rem(me, 2)
    y = lax.rem(me // 2, 2)
    x = me // 4
    nx, ny, nc = me + 4 - 8 * x, me + 2 - 4 * y, me + 1 - 2 * c
    first_chip, last_chip = x + y == 0, x + y == 2

    def rcopy(src, dst, ss, rs, to):
        return pltpu.make_async_remote_copy(
            src_ref=src, dst_ref=dst, send_sem=ss, recv_sem=rs, device_id={"tp": to}, device_id_type=MESH
        )

    def take(ref, sem):
        pltpu.make_async_copy(ref, ref, sem).wait()

    def load_gu(k, s, sem):
        rows = pl.ds(pl.multiple_of(k * T, T), T)
        pltpu.make_async_copy(gate_hbm.at[rows], guc.at[s, 0], sem).start()
        pltpu.make_async_copy(up_hbm.at[rows], guc.at[s, 1], sem).start()

    def load_chunk(k, s):
        rows = pl.ds(pl.multiple_of(k * T, T), T)
        pltpu.make_async_copy(dy_hbm.at[rows], dyc.at[s], in_sem.at[s]).start()
        load_gu(k, s, in_sem.at[s])

    def load_panel(m, s):
        cols = pl.ds(pl.multiple_of(m * T, T), T)
        pltpu.make_async_copy(x_hbm.at[:, cols], pan.at[s, 0], first_sem.at[s]).start()
        pltpu.make_async_copy(dy_hbm.at[:, cols], pan.at[s, 1], first_sem.at[s]).start()

    def load_w(g):
        own, kept = g % 2, g // 2
        h = c if own else 1 - c
        for ab in range(2):
            first, second = (x, y) if ab == 0 else (y, x)
            i = first if kept else 1 - first
            for jo in range(2):
                j = second if jo else 1 - second
                src = pl.ds(pl.multiple_of(h * 1024 + ab * 512 + i * 256 + j * 128, B), B)
                dst = pl.ds((g * 4 + jo * 2 + ab) * B, B)
                pltpu.make_async_copy(wg_hbm.at[src], wcat.at[dst, 0:F], w_sem.at[min(g, 2)]).start()
                pltpu.make_async_copy(wu_hbm.at[src], wcat.at[dst, F : 2 * F], w_sem.at[min(g, 2)]).start()

    def piece(ref, k, ab, cx, cy, h):
        col = h * 1024 + (cx * 256 + cy * 128 if ab == 0 else 512 + cy * 256 + cx * 128)
        return ref.at[pl.ds(pl.multiple_of(k * T, T), T), pl.ds(pl.multiple_of(col, B), B)]

    def c1_part(ref, k, part):
        return ref.at[k, 1] if part == 2 else ref.at[k, 0, pl.ds(part * 256, 256)]

    def c1_slot(k, part):
        return 4 + lax.rem(k, 4) if part == 2 else 2 * part + lax.rem(k, 2)

    def c1_send(k, part):
        rcopy(c1_part(c1s, k, part), c1_part(c1r, k, part), sent.at[1], c1_sem.at[c1_slot(k, part)], nc).start()

    def g_send(k, ab, kind):
        far, near = (ny, nx) if ab else (nx, ny)
        if kind == 2:
            ref = piece(dx, k, ab, x, 1 - y, c) if ab == 0 else piece(dx, k, ab, 1 - x, y, c)
        else:
            ref = piece(dx, k, ab, x, y, c)
        rcopy(ref, ref, sent.at[0], (p2_sem if kind == 2 else p1_sem).at[k], near if kind == 0 else far).start()

    def cf_send(k, ab, which, h=c, sem=1):
        cx, cy = ((x, y), (x, 1 - y), (1 - x, y), (1 - x, 1 - y))[which]
        ref = piece(dx, k, ab, cx, cy, h)
        rcopy(ref, ref, sent.at[sem], cf_sem, nc).start()

    def g_send_last(ab):
        cx, cy = (x, 1 - y) if ab == 0 else (1 - x, y)
        ref = piece(dx, NC - 1, ab, cx, cy, c)
        rcopy(ref, ref, sent.at[0], last_sem.at[ab], (ny if ab else nx) + 1 - c).start()

    def s1(k, jo):
        with jax.named_scope("s1"):
            take(c1_part(c1r, k, jo), c1_sem.at[c1_slot(k, jo)])
        for ab in range(2):
            rows = pl.ds(jo * 256 + ab * B, B)
            p1s[k, jo, ab] = (outs[rows] + c1r[k, 0, rows].astype(F32)).astype(BF)
            across, other = (ny, nx) if ab else (nx, ny)
            plain = rcopy(p1s.at[k, jo, ab], p1r.at[k, jo, ab], sent.at[0], p1_sem.at[k], across)
            if jo:
                skip = jnp.logical_and(k == VIA, last_chip)
            else:
                skip = jnp.logical_and(k == VIA, jnp.logical_and(x + y == 1, (y if ab else x) == 1))

                @pl.when(skip)
                def _():
                    part = p1s.at[k, jo, ab, pl.ds(0, RV)]
                    rcopy(part, extra.at[ab], sent.at[0], extra_sem, other).start()
                    rest = pl.ds(RV, B - RV)
                    src, dst = p1s.at[k, jo, ab, rest], p1r.at[k, jo, ab, rest]
                    rcopy(src, dst, sent.at[0], p1_sem.at[k], across).start()

            pl.when(jnp.logical_not(skip))(plain.start)

    def s1_late():
        @pl.when(last_chip)
        def _():
            with jax.named_scope("late"):
                take(extra, extra_sem)
            for ab in range(2):
                rows = pl.ds(256 + ab * B, RV)
                total = outs[rows] + c1r[VIA, 0, rows].astype(F32) + extra[ab].astype(F32)
                p1s[VIA, 1, ab, 0:RV] = total.astype(BF)
                rcopy(
                    p1s.at[VIA, 1, ab], p1r.at[VIA, 1, ab], sent.at[0], p1_sem.at[VIA], ny if ab else nx
                ).start()

    def s2(k):
        with jax.named_scope("s2"):
            take(c1r.at[k, 1], c1_sem.at[c1_slot(k, 2)])
        alone = jnp.logical_and(k == VIA, first_chip)

        def total(jo, ab):
            rows = pl.ds(jo * 256 + ab * B, B)
            return keep[k, rows] + c1r[k, 1, rows].astype(F32)

        def send(ab):
            rcopy(p2s.at[k, ab], p2r.at[k, ab], sent.at[0], p2_sem.at[k], nx if ab else ny).start()

        @pl.when(alone)
        def _():
            take(dcat.at[0 : 2 * (2 * B - RV) * T // 1024, 0:1024], p1_sem.at[k])
            for ab in range(2):
                mine = total(0, ab)
                p2s[k, ab, 0:RV] = mine[0:RV].astype(BF)
                p2s[k, ab, RV:B] = (mine[RV:B] + p1r[k, 0, ab, RV:B].astype(F32)).astype(BF)
                send(ab)

        @pl.when(jnp.logical_not(alone))
        def _():
            with jax.named_scope("s2"):
                take(p1r.at[k], p1_sem.at[k])
            for ab in range(2):
                p2s[k, ab] = (total(0, ab) + p1r[k, 0, ab].astype(F32)).astype(BF)
                send(ab)

        for ab in range(2):
            keep[k, pl.ds(256 + ab * B, B)] = total(1, ab) + p1r[k, 1, ab].astype(F32)

    @jax.named_scope("s3")
    def s3(k):
        take(p2r.at[k], p2_sem.at[k])
        for ab in range(2):
            done = (keep[k, pl.ds(256 + ab * B, B)] + p2r[k, ab].astype(F32)).astype(BF)
            piece(dx, k, ab, x, y, c)[...] = done.T
            g_send(k, ab, 0)
            g_send(k, ab, 1)
            cf_send(k, ab, 0)

    @jax.named_scope("s4")
    def s4(k):
        take(p1r.at[k], p1_sem.at[k])
        for ab in range(2):

            @pl.when(k < NC - 1)
            def _():
                g_send(k, ab, 2)

            @pl.when(k == NC - 1)
            def _():
                g_send_last(ab)

            cf_send(k, ab, 1)
            cf_send(k, ab, 2)

    @jax.named_scope("s5")
    def s5(k):
        @pl.when(k < NC - 1)
        def _():
            take(p2r.at[k], p2_sem.at[k])
            for ab in range(2):
                cf_send(k, ab, 3)

        @pl.when(jnp.logical_and(k == NC - 1, c == 1))
        def _():
            for ab in range(2):
                take(p2r.at[k], last_sem.at[ab])
                cf_send(k, ab, 3)
                cf_send(k, ab, 3, h=0, sem=2)

    def exchange(k, lag, fn):
        @pl.when(jnp.logical_and(k >= lag, k < NC + lag))
        def _():
            fn(k - lag)

    def gates(k, slot):
        cols = pl.ds(pl.multiple_of(k * T, T), T)
        for r in range(5):
            rows = slice(r * B, (r + 1) * B)
            g = guc[slot, 0, :, rows].T.astype(F32)
            u = guc[slot, 1, :, rows].T.astype(F32)
            g2 = g * g
            t = jnp.tanh(g * (C0 + (C0 * C1) * g2))
            cdf = 0.5 + 0.5 * t
            act = g * cdf
            slope = cdf + (act * (1.0 - t)) * (C0 + (3.0 * C0 * C1) * g2)
            hid[rows, cols] = (act * u).astype(BF)
            act_s[rows] = act
            slope_s[rows] = u * slope

    def store_grads(k, r, d):
        cols = pl.ds(pl.multiple_of(k * T, T), T)
        dcat[r, cols] = (d * slope_s[r]).astype(BF)
        dcat[F + r.start : F + r.stop, cols] = (d * act_s[r]).astype(BF)

    def halves(n):
        return [slice(i * n // 2, (i + 1) * n // 2) for i in range(2)]

    def term(k, rows):
        return dot(wcat[rows], dcat[:, pl.ds(pl.multiple_of(k * T, T), T)])

    parts = (slice(0, 512), slice(512, 1280), slice(1280, D))

    def load_first(i):
        d = parts[i]
        pltpu.make_async_copy(wd_hbm.at[:, d], wd.at[:, d], first_sem.at[i]).start()
        pltpu.make_async_copy(dy_hbm.at[0:T, d], dyc.at[0, :, d], first_sem.at[i]).start()

    def grads(k, slot, parts, i):
        with jax.named_scope("grads"):
            if not i:
                gates(k, slot)
            for r in halves(F):
                part = dot(wd[r, parts[i]], dyc[slot, :, parts[i]], ((1,), (1,)))
                total = dh[r] + part if i else part
                if i == len(parts) - 1:
                    store_grads(k, r, total)
                else:
                    dh[r] = total

    load_first(0)
    load_gu(0, 0, first_sem.at[0])
    barrier = pltpu.get_barrier_semaphore()
    for to in (nx, ny, nc, nx + 1 - 2 * c, ny + 1 - 2 * c):
        pl.semaphore_signal(barrier, inc=1, device_id={"tp": to}, device_id_type=MESH)
    pl.delay(250)
    load_first(1)
    pl.delay(250)
    load_first(2)
    pl.delay(250)
    load_w(0)
    for i, d in enumerate(parts):
        with jax.named_scope("load"):
            n = (T + F) * (d.stop - d.start) + (0 if i else 2 * T * F)
            take(dcat.at[0 : n // 1024, 0:1024], first_sem.at[i])
        if not i:
            load_w(1)
            load_chunk(1, 1)
        grads(0, 0, parts, i)
    load_w(2)
    load_w(3)
    with jax.named_scope("bar"):
        pl.semaphore_wait(barrier, 5)

    def first_use(k, g):
        @pl.when(k == 0)
        def _():
            take(wcat.at[g * 512 : 2048 if g == 2 else (g + 1) * 512], w_sem.at[g])

    def keep_partner(k):
        first_use(k, 2)
        with jax.named_scope("keeps"):
            for r in halves(512):
                c1s[k, 1, r] = term(k, slice(1024 + r.start, 1024 + r.stop)).astype(BF)
        c1_send(k, 2)

    def keep_own(k):
        with jax.named_scope("keeps"):
            for r in halves(512):
                keep[k, r] = term(k, slice(1536 + r.start, 1536 + r.stop))

    def phase1(k, _):
        first_use(k, 0)
        for ab in range(2):
            with jax.named_scope("termP"):
                for i in range(2):
                    r = slice(ab * 256 + i * 128, ab * 256 + (i + 1) * 128)
                    c1s[k, 0, r] = term(k, r).astype(BF)
            c1_send(k, ab)
        first_use(k, 1)
        with jax.named_scope("out"):
            for r in halves(512):
                outs[r] = term(k, slice(512 + r.start, 512 + r.stop))
        s1(k, 0)

        @pl.when(k >= L1)
        def _():
            keep_partner(k - L1)

        nxt = k + 1
        slot = lax.rem(nxt, 2)

        @pl.when(k < NC - 1)
        def _():
            take(dcat.at[0 : (T * D + 2 * T * F) // D], in_sem.at[slot])
            grads(nxt, slot, (slice(0, D),), 0)

            @pl.when(nxt < NC - 1)
            def _():
                load_chunk(nxt + 1, 1 - slot)

            @pl.when(jnp.logical_and(k >= 2, k < 4))
            def _():
                load_panel(k - 2, k - 2)

        s1(k, 1)

        @pl.when(k >= L1)
        def _():
            keep_own(k - L1)

        exchange(k, L2, s2)
        exchange(k, L3, s3)
        exchange(k, L4, s4)
        exchange(k, L5, s5)
        return 0

    lax.fori_loop(0, NC, phase1, 0)

    def last_keeps(k, _):
        keep_partner(k)
        keep_own(k)
        return 0

    lax.fori_loop(NC - L1, NC, last_keeps, 0)

    def phase2(m, _):
        slot = lax.rem(m, 2)
        k = NC + m
        at = pl.ds(pl.multiple_of(m * T, T), T)
        take(pan.at[slot], first_sem.at[slot])
        with jax.named_scope("dwg"):
            for r in halves(F):
                dwg[at, r] = dot(dcat[r], pan[slot, 0]).astype(BF).T
        pl.when(m == 0)(s1_late)
        exchange(k, L2, s2)
        with jax.named_scope("dwu"):
            for r in halves(F):
                dwu[at, r] = dot(dcat[F + r.start : F + r.stop], pan[slot, 0]).astype(BF).T
        exchange(k, L3, s3)
        exchange(k, L4, s4)
        with jax.named_scope("dwd"):
            for r in halves(F):
                dwd[r, at] = dot(hid[r], pan[slot, 1]).astype(BF)

        @pl.when(m < NC - 2)
        def _():
            load_panel(m + 2, slot)

        exchange(k, L5, s5)
        return 0

    lax.fori_loop(0, NC, phase2, 0)

    def phase3(k, _):
        exchange(k, L4, s4)
        exchange(k, L5, s5)
        return 0

    lax.fori_loop(2 * NC, NC + L5, phase3, 0)
    with jax.named_scope("fin"):
        take(dx.at[0:1536], sent.at[0])

        @pl.when(c == 0)
        def _():
            take(dx.at[0:2016], sent.at[1])
            take(dx.at[0:1056], cf_sem)

        @pl.when(c == 1)
        def _():
            take(dx, sent.at[1])
            take(dx.at[0:32], sent.at[2])
            take(dx.at[0:992], cf_sem)


def write_out(dx, dwg, dwu, dwd, dx_o, dwg_o, dwu_o, dwd_o, sem):
    pairs = ((dx, dx_o, 4), (dwg, dwg_o, 2), (dwu, dwu_o, 2), (dwd, dwd_o, 2))
    for k, (src, dst, parts) in enumerate(pairs):
        n = src.shape[0] // parts
        for i in range(parts):
            rows = pl.ds(i * n, n)
            pltpu.make_async_copy(src.at[rows], dst.at[rows], sem.at[k]).start()
    for k, (src, dst, _) in enumerate(pairs):
        pltpu.make_async_copy(src, dst, sem.at[k]).wait()


def solution(mesh):
    def step(x, dy, gate, up, w_gate, w_up, w_down):
        hbm = pl.BlockSpec(memory_space=pltpu.HBM)
        vmem = pl.BlockSpec(memory_space=pltpu.VMEM)
        shapes = ((D, D), (D, F), (D, F), (F, D))
        dma = pltpu.SemaphoreType.DMA
        args = [pltpu.with_memory_space_constraint(a, pltpu.HBM) for a in (x, dy, gate, up, w_gate, w_up, w_down)]
        results = pl.pallas_call(
            kernel,
            out_shape=tuple(pltpu.VMEM(s, BF) for s in shapes),
            in_specs=[hbm] * 7,
            out_specs=(vmem,) * 4,
            scratch_shapes=[
                pltpu.VMEM((D, 2 * F), BF),
                pltpu.VMEM((F, D), BF),
                pltpu.VMEM((2 * F, D), BF),
                pltpu.VMEM((F, D), BF),
                pltpu.VMEM((2, T, D), BF),
                pltpu.VMEM((2, 2, T, F), BF),
                pltpu.VMEM((2, 2, D, T), BF),
                pltpu.VMEM((F, T), F32),
                pltpu.VMEM((F, T), F32),
                pltpu.VMEM((F, T), F32),
                pltpu.VMEM((NC, 512, T), F32),
                pltpu.VMEM((512, T), F32),
                pltpu.VMEM((NC, 2, 512, T), BF),
                pltpu.VMEM((NC, 2, 512, T), BF),
                pltpu.VMEM((NC, 2, 2, B, T), BF),
                pltpu.VMEM((NC, 2, 2, B, T), BF),
                pltpu.VMEM((NC, 2, 128, T), BF),
                pltpu.VMEM((NC, 2, 128, T), BF),
                pltpu.VMEM((2, RV, T), BF),
                dma((2,)),
                dma((3,)),
                dma((3,)),
                dma((8,)),
                dma((NC,)),
                dma((NC,)),
                dma,
                dma((3,)),
                dma,
                dma((2,)),
            ],
            compiler_params=pltpu.CompilerParams(
                collective_id=0, has_side_effects=True, vmem_limit_bytes=48 * 2**20
            ),
        )(*args)
        return pl.pallas_call(
            write_out,
            out_shape=tuple(jax.ShapeDtypeStruct(s, BF) for s in shapes),
            in_specs=[vmem] * 4,
            out_specs=(hbm,) * 4,
            scratch_shapes=[dma((4,))],
            compiler_params=pltpu.CompilerParams(vmem_limit_bytes=2**20),
        )(*results)

    tokens, columns, rows = P("dp", None), P(None, "tp"), P("tp", None)
    return jax.shard_map(
        step,
        mesh=mesh,
        in_specs=(tokens, tokens, P("dp", "tp"), P("dp", "tp"), columns, columns, rows),
        out_specs=(tokens, P("dp", "tp"), P("dp", "tp"), P(("dp", "tp"), None)),
        check_vma=False,
    )
```
